32 devices in a mesh: lat: 8 (over z, y), chan: 4 (over x, core).
Axes of the slice: x: 2, y: 2, z: 4, core: 2. Of those that a mesh axis runs over, the one named last changes fastest.
Arguments:
- grid_in: bfloat16 [256, 384, 1024], P('chan', 'lat'), may hold values from -6 to 6
- quad_weights: float32 [384], P('lat'), may hold values from 0.5 to 2
- legendre: bfloat16 [384, 384, 384], P('lat'), as said below
- mixing: bfloat16 [2, 384, 256, 256], P(None, 'lat', 'chan'), may hold values from -0.375 to 0.375
Outputs:
- grid_out: bfloat16 [256, 384, 1024], P('chan', 'lat')
The draws below stay inside these ranges and needn't reach their ends.
Inputs may be any that keep to these rules, and one draw needn't show every extreme that they name: legendre[m, l, t] is zero wherever l < m.
All inputs are finite; a program needn't handle non-finite values.
Results may differ from the reference program's by a relative error of at most 0.0068.
Values may be sent and summed in bfloat16 or wider, within the bound.
A program may use at most 128 MiB of HBM per device.

```python
import math
import jax
import jax.numpy as jnp
from jax import lax

C = 256
NLAT = 384
NLON = 1024
M = 384
L = 384


def draw_legendre(key, part):
    values = jax.random.normal(key, (M, L, NLAT), jnp.float32)
    orders = jnp.arange(M, dtype=jnp.int32)[:, None, None]
    degrees = jnp.arange(L, dtype=jnp.int32)[None, :, None]
    values = jnp.where(degrees >= orders, values, 0.0) * NLAT ** (-0.5)
    return values.astype(jnp.bfloat16)


def spiked(array, own_key, source, target, parts, factor):
    def block_of(axis_at):
        return (jnp.arange(array.shape[axis_at]) // (array.shape[axis_at] // parts)).reshape((-1,) + (1,) * (array.ndim - 1 - axis_at))

    one_side = jax.random.permutation(own_key, parts)[block_of(target)]
    second = (block_of(target) + parts // 2) % parts
    return jnp.where((block_of(source) == one_side) | (block_of(source) == second), factor * array, array)


def levels(rng, dims, pieces, smallest, largest):
    gain = 1.0
    for dim, shards_of in pieces:
        heights = jax.random.uniform(jax.random.fold_in(jax.random.fold_in(rng, 6), dim), (shards_of,), jnp.float32, smallest / len(pieces), largest / len(pieces))
        gain = gain * jnp.repeat(jnp.exp(heights), dims[dim] // shards_of).reshape((-1,) + (1,) * (len(dims) - 1 - dim))
    return gain


def gaussian(stream_key, extent, scale, limit, split=(), held_as=jnp.bfloat16):
    factor_of = levels(stream_key, extent, split, -0.22, 0.18) if split else 1.0
    drawn = jax.random.normal(stream_key, extent, jnp.float32) * scale * factor_of
    return jnp.minimum(jnp.maximum(drawn, -limit), limit).astype(held_as)


def noise_with(own_key, extent, scale, reach, cuts, heavy, kind=jnp.bfloat16):
    array = scale * jax.random.normal(own_key, extent, jnp.float32)
    if cuts:
        array = array * levels(own_key, extent, cuts, -0.22, 0.18)
    return jnp.clip(spiked(array, jax.random.fold_in(own_key, 3), *heavy), -reach, reach).astype(kind)


def setup_inputs(seed: int = 0) -> dict:
    arg_keys = jax.random.split(jax.random.key(seed), 5)
    grid_in = gaussian(arg_keys[0], (C, NLAT, NLON), 1.0, 6.0, ((0, 4), (1, 8)))
    quad_weights = jnp.clip(jnp.exp(math.log(2.0) - 1.3862944 * jax.random.uniform(arg_keys[1], (NLAT,), jnp.float32) ** levels(arg_keys[1], (NLAT,), ((0, 8),), -0.2, 0.2)), 0.5, 2.0)
    legendre = draw_legendre(jax.random.fold_in(arg_keys[4], 71), 0)
    mixing = noise_with(arg_keys[3], (2, L, C, C), (2 * C) ** -0.5, 0.375, ((1, 8), (2, 4)), (2, 3, 4, 2.0))
    return {"grid_in": grid_in, "quad_weights": quad_weights, "legendre": legendre, "mixing": mixing}


def fourier_table(number, length):
    orders = jnp.arange(number, dtype=jnp.int32)
    points = jnp.arange(length, dtype=jnp.int32)
    phases = orders[:, None] * points[None, :] % length
    angles = phases.astype(jnp.float32) * (2.0 * math.pi / length)
    factor = 1.0 / math.sqrt(length)
    return jnp.stack([jnp.cos(angles) * factor, -jnp.sin(angles) * factor]).astype(jnp.bfloat16)

def reference(grid_in, quad_weights, legendre, mixing):
    fourier = fourier_table(M, NLON)
    flattened = grid_in.reshape(C * NLAT, NLON)
    spectra = jnp.dot(flattened, fourier.reshape(2 * M, NLON).T, preferred_element_type=jnp.float32)
    spectra = spectra.reshape(C, NLAT, 2, M) * quad_weights[None, :, None, None]
    weighted = spectra.astype(jnp.bfloat16).transpose(3, 1, 2, 0).reshape(M, NLAT, 2 * C)

    def forward_one(operands):
        return jnp.dot(operands[0], operands[1], preferred_element_type=jnp.float32).astype(jnp.bfloat16)
    coeffs = lax.map(forward_one, (legendre, weighted))
    by_degree = coeffs.transpose(1, 0, 2)
    weights_by = mixing.transpose(1, 0, 2, 3)

    def mix_one(operands):
        values, weight = operands
        real_in = values[:, :C]
        imag_in = values[:, C:]
        real_out = jnp.dot(real_in, weight[0], preferred_element_type=jnp.float32) - jnp.dot(imag_in, weight[1], preferred_element_type=jnp.float32)
        imag_out = jnp.dot(imag_in, weight[0], preferred_element_type=jnp.float32) + jnp.dot(real_in, weight[1], preferred_element_type=jnp.float32)
        return jnp.concatenate([real_out, imag_out], axis=1).astype(jnp.bfloat16)
    mixed_coef = lax.map(mix_one, (by_degree, weights_by)).transpose(1, 0, 2)

    def inverse_one(operands):
        return jnp.dot(operands[0].T, operands[1], preferred_element_type=jnp.float32).astype(jnp.bfloat16)
    synthesis = lax.map(inverse_one, (legendre, mixed_coef))
    spread = synthesis.reshape(M, NLAT, 2, C).transpose(3, 1, 2, 0).reshape(C * NLAT, 2 * M)
    restored = jnp.dot(spread, fourier.reshape(2 * M, NLON), preferred_element_type=jnp.float32)
    return (restored.reshape(C, NLAT, NLON) + grid_in.astype(jnp.float32)).astype(jnp.bfloat16)
```

```python
import functools
import math

import jax
import jax.numpy as jnp
from jax import lax
from jax.experimental import pallas as pl
from jax.experimental.pallas import tpu as pltpu
from jax.sharding import PartitionSpec as P

M = 384
PIECES = (2, 1)


def fourier_table(number, length):
    orders = jnp.arange(number, dtype=jnp.int32)
    points = jnp.arange(length, dtype=jnp.int32)
    phases = orders[:, None] * points[None, :] % length
    angles = phases.astype(jnp.float32) * (2.0 * math.pi / length)
    factor = 1.0 / math.sqrt(length)
    return jnp.stack([jnp.cos(angles) * factor, -jnp.sin(angles) * factor]).astype(jnp.bfloat16)


def step_of(part):
    return next(count for count in (4, 3, 2, 1) if part % count == 0)


def price(legendre, columns):
    orders, degrees, points = legendre.shape
    return pl.CostEstimate(
        flops=2 * orders * degrees * points * columns,
        bytes_accessed=2 * orders * (degrees * points + (degrees + points) * columns),
        transcendentals=0,
    )


def analyse(legendre, gathered, chans):
    lats, orders, rows_lat, columns = gathered.shape
    degrees = legendre.shape[1] // lats
    part = orders // chans
    step = step_of(part)
    runs = part // step

    def kernel(table_ref, values_ref, out_ref):
        for at in range(step):
            values = values_ref[:, at].reshape(lats * rows_lat, columns)
            sums = jnp.dot(table_ref[at], values, preferred_element_type=jnp.float32)
            out_ref[:, 0, at] = sums.astype(jnp.bfloat16).reshape(lats, degrees, columns)

    return pl.pallas_call(
        kernel,
        grid=(orders // step,),
        in_specs=[
            pl.BlockSpec((step,) + legendre.shape[1:], lambda g: (g, 0, 0)),
            pl.BlockSpec((lats, step, rows_lat, columns), lambda g: (0, g, 0, 0)),
        ],
        out_specs=pl.BlockSpec(
            (lats, 1, step, degrees, columns), lambda g: (0, g // runs, g % runs, 0, 0)
        ),
        out_shape=jax.ShapeDtypeStruct((lats, chans, part, degrees, columns), jnp.bfloat16),
        cost_estimate=price(legendre, columns),
    )(legendre, gathered)


def synthesise(legendre, returned, rows_lat):
    lats, chans, part, degrees, columns = returned.shape
    orders = legendre.shape[0]
    step = step_of(part)
    runs = part // step

    def kernel(table_ref, values_ref, out_ref):
        for at in range(step):
            values = values_ref[:, 0, at].reshape(lats * degrees, columns)
            sums = lax.dot_general(
                table_ref[at],
                values,
                (((0,), (0,)), ((), ())),
                preferred_element_type=jnp.float32,
            )
            out_ref[:, at] = sums.astype(jnp.bfloat16).reshape(lats, rows_lat, columns)

    return pl.pallas_call(
        kernel,
        grid=(orders // step,),
        in_specs=[
            pl.BlockSpec((step,) + legendre.shape[1:], lambda g: (g, 0, 0)),
            pl.BlockSpec(
                (lats, 1, step, degrees, columns), lambda g: (0, g // runs, g % runs, 0, 0)
            ),
        ],
        out_specs=pl.BlockSpec((lats, step, rows_lat, columns), lambda g: (0, g, 0, 0)),
        out_shape=jax.ShapeDtypeStruct((lats, orders, rows_lat, columns), jnp.bfloat16),
        cost_estimate=price(legendre, columns),
    )(legendre, returned)


def general(chans, grid_in, quad_weights, legendre, mixing):
    groups = grid_in.shape[0]
    rows_lat = grid_in.shape[1]
    length = grid_in.shape[2]
    orders = legendre.shape[0]
    degrees = mixing.shape[1]
    lats = legendre.shape[1] // degrees
    part = -(-orders // chans)
    padding = part * chans - orders
    everyone = ("lat", "chan")

    channel = jnp.arange(chans * groups)
    place = channel // groups * (2 * groups) + channel % groups
    column = jnp.arange(2 * chans * groups)
    to_real = (column == place[:, None]).astype(jnp.bfloat16)
    to_imag = (column == place[:, None] + groups).astype(jnp.bfloat16)

    def spread_out(table):
        return jnp.einsum(
            "rlcd,rdy->lcy", mixing, table, preferred_element_type=jnp.float32
        ).astype(jnp.bfloat16)

    blocks = jnp.concatenate(
        [
            spread_out(jnp.stack([to_real, to_imag])),
            spread_out(jnp.stack([to_imag, -to_real])),
        ],
        axis=1,
    )
    weights = lax.all_gather(blocks, "chan", axis=0)
    fourier = fourier_table(M, length)
    spectra = jnp.einsum("ctn,rmn->mtrc", grid_in, fourier, preferred_element_type=jnp.float32)
    spectra = spectra * quad_weights[None, :, None, None]
    weighted = spectra.astype(jnp.bfloat16).reshape(M, rows_lat, 2 * groups)
    gathered = lax.all_to_all(weighted, "lat", split_axis=0, concat_axis=0, tiled=True)
    gathered = gathered.reshape(lats, orders, rows_lat, 2 * groups)
    fits = padding == 0 and rows_lat % 16 == 0 and degrees % 16 == 0
    if fits:
        outgoing = analyse(legendre, gathered, chans)
    else:
        whole = gathered.transpose(1, 0, 2, 3).reshape(orders, lats * rows_lat, 2 * groups)
        coeffs = jnp.einsum(
            "mlt,mtk->mlk", legendre, whole, preferred_element_type=jnp.float32
        ).astype(jnp.bfloat16)
        coeffs = jnp.pad(coeffs, ((0, padding), (0, 0), (0, 0)))
        outgoing = coeffs.reshape(chans, part, lats, degrees, 2 * groups)
        outgoing = outgoing.transpose(2, 0, 1, 3, 4)
    pieces = next(count for count in PIECES if part % count == 0)
    width = part // pieces
    place_lat = lax.axis_index("lat")
    peers = jnp.arange(lats).reshape(lats, 1, 1, 1, 1)

    def exchange(buffer, axes):
        flat = buffer.reshape((-1,) + buffer.shape[-3:])
        flat = lax.all_to_all(flat, axes, split_axis=0, concat_axis=0, tiled=True)
        return flat.reshape(buffer.shape)

    def mix(arrived):
        mixed = jnp.einsum(
            "ikmlx,klxy->limy", arrived, weights, preferred_element_type=jnp.float32
        ).astype(jnp.bfloat16)
        mixed = mixed.reshape(degrees, lats, width, chans, 2 * groups)
        return mixed.transpose(1, 3, 2, 0, 4)

    received = [exchange(outgoing[:, :, :width], ("lat", "chan"))]
    own = []
    for piece in range(1, pieces + 1):
        mixed = mix(received[-1])
        if piece < pieces:
            own.append(lax.dynamic_index_in_dim(mixed, place_lat, 0, keepdims=False))
            coming = outgoing[:, :, piece * width : (piece + 1) * width]
            mixed = jnp.where(peers >= place_lat, coming, mixed)
        received.append(exchange(mixed, ("lat", "chan")))
    if own:
        own = exchange(jnp.concatenate(own, axis=1), "chan")
    returned = []
    for piece in range(pieces):
        block = received[piece + 1]
        if piece < pieces - 1:
            mine = own[None, :, piece * width : (piece + 1) * width]
            block = jnp.where(peers == place_lat, mine, block)
        returned.append(jnp.where(peers >= place_lat, block, jnp.zeros_like(block)))
    returned = jnp.concatenate(returned, axis=2)
    if fits:
        synthesis = synthesise(legendre, returned, rows_lat)
    else:
        mixed_coef = returned.transpose(1, 2, 0, 3, 4)
        mixed_coef = mixed_coef.reshape(chans * part, lats * degrees, 2 * groups)[:orders]
        synthesis = jnp.einsum(
            "mlt,mlk->mtk", legendre, mixed_coef, preferred_element_type=jnp.float32
        ).astype(jnp.bfloat16)
        synthesis = synthesis.reshape(orders, lats, rows_lat, 2 * groups).transpose(1, 0, 2, 3)
    synthesis = synthesis.reshape(lats * orders, rows_lat, 2 * groups)
    gridded = lax.all_to_all(synthesis, "lat", split_axis=0, concat_axis=0, tiled=True)
    spread = gridded.reshape(M, rows_lat, 2, groups)
    restored = jnp.einsum("mtrc,rmn->ctn", spread, fourier, preferred_element_type=jnp.float32)
    return (restored + grid_in.astype(jnp.float32)).astype(jnp.bfloat16)


MESH = pl.DeviceIdType.MESH
LANES = 128


def chunks_of(orders, chans):
    return next((count for count in (4, 3, 2, 1) if orders % (count * chans) == 0), 0)


def exchange_kernel(
    lats, chans, chunks,
    leg, outgoing, mix, arrived, weights,
    w_recv, c_send, c_recv, x_send, x_recv, s_send,
    legs, tiles, fa, fb,
    leg_sem, tile_sem, own_sem,
    ws_sem, wr_sem, cs_sem, cr_sem, xs_sem, xr_sem, ss_sem, sr_sem, gs_sem, gr_sem,
):
    here = lax.axis_index("lat")
    group = lax.axis_index("chan")
    orders, degrees_all, points_all = leg.shape
    degrees = degrees_all // lats
    points = points_all // lats
    size = orders // chunks
    part = size // chans
    rows = lats * part
    columns = outgoing.shape[-1]
    span = tiles.shape[1]
    bands = degrees // span
    inner = tiles.shape[3] // chans
    wide = chans * columns // 2

    def to(lat, chan):
        return {"device_id": {"lat": lat, "chan": chan}, "device_id_type": MESH}

    def each_peer(do):
        def step(d, carry):
            do(lax.rem(here + d, lats))
            return carry

        lax.fori_loop(1, lats, step, 0)

    def each_pair(low, high, do):
        def step(n, carry):
            lat = n // chans
            chan = n % chans

            @pl.when(jnp.logical_or(lat != here, chan != group))
            def _():
                do(lat, chan)

            return carry

        lax.fori_loop(low * chans, high * chans, step, 0)

    def weighted_copy(j, peer, source):
        at = pl.ds(j * size, size)
        return pltpu.make_async_remote_copy(
            src_ref=outgoing.at[peer, at], dst_ref=w_recv.at[source, at],
            send_sem=ws_sem.at[j, peer], recv_sem=wr_sem.at[j, source],
            **to(peer, group),
        )

    def send_weighted(j):
        each_peer(lambda peer: weighted_copy(j, peer, here).start())

    def own_weighted():
        return pltpu.make_async_copy(outgoing.at[here], w_recv.at[here], own_sem.at[0])

    def coeff_copy(j, lat, chan, from_lat, from_chan):
        at = pl.ds(j * part, part)
        return pltpu.make_async_remote_copy(
            src_ref=c_send.at[lat, chan, at], dst_ref=c_recv.at[from_lat, from_chan, at],
            send_sem=cs_sem.at[j, lat, chan], recv_sem=cr_sem.at[j, from_lat, from_chan],
            **to(lat, chan),
        )

    def mixed_copy(j, lat, chan, from_lat, from_chan):
        at = pl.ds(j * part, part)
        return pltpu.make_async_remote_copy(
            src_ref=x_send.at[lat, chan, at], dst_ref=x_recv.at[from_lat, from_chan, at],
            send_sem=xs_sem.at[j, lat, chan], recv_sem=xr_sem.at[j, from_lat, from_chan],
            **to(lat, chan),
        )

    def synthesis_copy(j, peer, source):
        at = pl.ds(j * size, size)
        return pltpu.make_async_remote_copy(
            src_ref=s_send.at[peer, at], dst_ref=arrived.at[source, at],
            send_sem=ss_sem.at[j, peer], recv_sem=sr_sem.at[j, source],
            **to(peer, group),
        )

    def own_synthesis(j):
        at = pl.ds(j * size, size)
        return pltpu.make_async_copy(s_send.at[here, at], arrived.at[here, at], own_sem.at[1])

    def leg_copy(use, j):
        return pltpu.make_async_copy(leg.at[pl.ds(j * size, size)], legs.at[use % 2], leg_sem.at[use % 2])

    def analyse(use, j):
        def step(n, carry):
            at = j * size + n
            values = w_recv[:, at].reshape(lats * points, columns)
            sums = jnp.dot(legs[use % 2, n], values, preferred_element_type=jnp.float32)
            c_send[:, n // part, j * part + n % part] = sums.astype(jnp.bfloat16).reshape(lats, degrees, columns)
            return carry

        lax.fori_loop(0, size, step, 0)
        at = pl.ds(j * part, part)
        each_pair(here, lats, lambda lat, chan: coeff_copy(j, lat, chan, here, group).start())
        c_recv[here, group, at] = c_send[here, group, at]

    def synthesise(use, j):
        def step(n, carry):
            values = x_recv[:, n // part, j * part + n % part].reshape(lats * degrees, columns)
            sums = lax.dot_general(
                legs[use % 2, n], values, (((0,), (0,)), ((), ())), preferred_element_type=jnp.float32
            )
            s_send[:, j * size + n] = sums.astype(jnp.bfloat16).reshape(lats, points, columns)
            return carry

        lax.fori_loop(0, size, step, 0)
        each_peer(lambda peer: synthesis_copy(j, peer, here).start())
        own_synthesis(j).start()
        own_synthesis(j).wait()

    def tile_copies(band, slot, do):
        at = pl.ds(band * span, span)
        for chan in range(chans):
            for r in range(2):
                target = tiles.at[slot, :, r, pl.ds(chan * inner, inner)]
                sem = tile_sem.at[slot, chan, r]

                @pl.when(chan == group)
                def _():
                    do(pltpu.make_async_copy(mix.at[r, at], target, sem))

                @pl.when(chan != group)
                def _():
                    do(pltpu.make_async_copy(weights.at[chan, r, at], target, sem))

    def mix_chunk(j):
        at = pl.ds(j * part, part)
        block = part * degrees
        tile_copies(0, 0, lambda copy: copy.start())

        def widen(s, carry):
            for chan in range(chans):
                values = c_recv[s, chan, at].astype(jnp.float32)
                fa[chan, pl.ds(s * block, block)] = values.reshape(block, columns)
            return carry

        lax.fori_loop(0, lats, widen, 0)
        half = columns // 2
        lane = lax.broadcasted_iota(jnp.int32, (rows, columns), 1) < half

        def band_step(band, carry):
            slot = band % 2

            @pl.when(band + 1 < bands)
            def _():
                tile_copies(band + 1, 1 - slot, lambda copy: copy.start())

            tile_copies(band, slot, lambda copy: copy.wait())

            def degree_step(n, carry):
                picked = pl.ds(band * span + n, rows, stride=degrees)
                taken = [fa[chan, picked, :] for chan in range(chans)]
                real, imag = [], []
                for low, high in zip(taken[0::2], taken[1::2]):
                    real.append(jnp.where(lane, low, pltpu.roll(high, half, 1)))
                    imag.append(jnp.where(lane, pltpu.roll(low, half, 1), high))
                stacked = jnp.concatenate(
                    [jnp.concatenate(real, axis=1), jnp.concatenate(imag, axis=1)], axis=0
                ).astype(jnp.bfloat16)
                by_real = jnp.dot(stacked, tiles[slot, n, 0], preferred_element_type=jnp.float32)
                by_imag = jnp.dot(stacked, tiles[slot, n, 1], preferred_element_type=jnp.float32)
                real_out = by_real[:rows] - by_imag[rows:]
                imag_out = by_real[rows:] + by_imag[:rows]
                for pair in range(chans // 2):
                    first = real_out[:, pair * columns : (pair + 1) * columns]
                    second = imag_out[:, pair * columns : (pair + 1) * columns]
                    fb[2 * pair, picked, :] = jnp.where(lane, first, pltpu.roll(second, half, 1))
                    fb[2 * pair + 1, picked, :] = jnp.where(lane, pltpu.roll(first, half, 1), second)
                return carry

            lax.fori_loop(0, span, degree_step, 0)
            return carry

        lax.fori_loop(0, bands, band_step, 0)

        def narrow(s, carry):
            for chan in range(chans):
                values = fb[chan, pl.ds(s * block, block)].astype(jnp.bfloat16)
                x_send[s, chan, at] = values.reshape(part, degrees, columns)
            return carry

        lax.fori_loop(0, here + 1, narrow, 0)
        each_pair(0, here + 1, lambda lat, chan: mixed_copy(j, lat, chan, here, group).start())
        x_recv[here, group, at] = x_send[here, group, at]

    steps = []
    distance = chans // 2
    held = 1
    while distance:
        steps.append(distance)
        distance //= 2

    def gather_copies(level):
        distance = steps[level]
        peer = jnp.bitwise_xor(group, distance)
        copies = []
        for n in range(2**level):
            offset = sum(steps[b] for b in range(level) if n >> b & 1)
            shard = jnp.bitwise_xor(group, offset)
            source = mix if offset == 0 else weights.at[shard]
            copies.append(
                pltpu.make_async_remote_copy(
                    src_ref=source, dst_ref=weights.at[shard],
                    send_sem=gs_sem.at[level, n], recv_sem=gr_sem.at[level, n],
                    **to(here, peer),
                )
            )
        return copies

    use = 0
    order = []
    plan = []
    for j in range(chunks):
        plan.append(("L", j))
        if j >= 1:
            plan.append(("X", j - 1))
        if j >= 2:
            plan.append(("S", j - 2))
    plan.append(("X", chunks - 1))
    if chunks >= 2:
        plan.append(("S", chunks - 2))
    plan.append(("S", chunks - 1))
    order = [(kind, j) for kind, j in plan if kind != "X"]

    leg_copy(0, order[0][1]).start()
    own_weighted().start()
    for j in range(min(2, chunks)):
        send_weighted(j)
    for copy in gather_copies(0):
        copy.start()

    def clear(s, carry):
        x_recv[s] = jnp.zeros(x_recv.shape[1:], x_recv.dtype)
        return carry

    lax.fori_loop(0, here, clear, 0)
    own_weighted().wait()

    use = 0
    gathered = False
    for kind, j in plan:
        if kind == "X":
            if not gathered:
                for level in range(len(steps)):
                    for copy in gather_copies(level):
                        copy.wait_recv()
                    if level + 1 < len(steps):
                        for copy in gather_copies(level + 1):
                            copy.start()
                gathered = True
            each_pair(0, here + 1, lambda lat, chan: coeff_copy(j, here, group, lat, chan).wait_recv())
            mix_chunk(j)
            continue
        if use + 1 < len(order):
            leg_copy(use + 1, order[use + 1][1]).start()
        if kind == "L":
            each_peer(lambda peer: weighted_copy(j, here, peer).wait_recv())
            leg_copy(use, j).wait()
            analyse(use, j)
            if j + 2 < chunks:
                send_weighted(j + 2)
        else:
            each_pair(here, lats, lambda lat, chan: mixed_copy(j, here, group, lat, chan).wait_recv())
            leg_copy(use, j).wait()
            synthesise(use, j)
        use += 1

    for level in range(len(steps)):
        for copy in gather_copies(level):
            copy.wait_send()
    for j in range(chunks):
        each_peer(lambda peer: weighted_copy(j, peer, here).wait_send())
        each_pair(here, lats, lambda lat, chan: coeff_copy(j, lat, chan, here, group).wait_send())
        each_pair(0, here + 1, lambda lat, chan: mixed_copy(j, lat, chan, here, group).wait_send())
    for j in range(chunks):
        each_peer(lambda peer: synthesis_copy(j, here, peer).wait_recv())
        each_peer(lambda peer: synthesis_copy(j, peer, here).wait_send())


def exchange(chans, chunks, legendre, outgoing, mixing):
    lats, orders, points, columns = outgoing.shape
    degrees = mixing.shape[1]
    size = orders // chunks
    part = size // chans
    rows = lats * part
    span = next(count for count in (8, 6, 4, 3, 2, 1) if degrees % count == 0)
    inner = mixing.shape[2]
    levels = max(1, chans.bit_length() - 1)
    spectral = (lats, chans, orders // chans, degrees, columns)
    gridded = (lats, orders, points, columns)
    half = jnp.bfloat16
    dma = pltpu.SemaphoreType.DMA
    arrived, _ = pl.pallas_call(
        functools.partial(exchange_kernel, lats, chans, chunks),
        in_specs=[pl.BlockSpec(memory_space=pl.ANY)] * 3,
        out_specs=[pl.BlockSpec(memory_space=pl.ANY)] * 2,
        out_shape=[
            jax.ShapeDtypeStruct(gridded, half),
            jax.ShapeDtypeStruct((chans,) + mixing.shape, half),
        ],
        scratch_shapes=[
            pltpu.VMEM(gridded, half),
            pltpu.VMEM(spectral, half),
            pltpu.VMEM(spectral, half),
            pltpu.VMEM(spectral, half),
            pltpu.VMEM(spectral, half),
            pltpu.VMEM(gridded, half),
            pltpu.VMEM((2, size) + legendre.shape[1:], half),
            pltpu.VMEM((2, span, 2, chans * inner, mixing.shape[3]), half),
            pltpu.VMEM((chans, rows * degrees, columns), jnp.float32),
            pltpu.VMEM((chans, rows * degrees, columns), jnp.float32),
            dma((2,)),
            dma((2, chans, 2)),
            dma((2,)),
            dma((chunks, lats)),
            dma((chunks, lats)),
            dma((chunks, lats, chans)),
            dma((chunks, lats, chans)),
            dma((chunks, lats, chans)),
            dma((chunks, lats, chans)),
            dma((chunks, lats)),
            dma((chunks, lats)),
            dma((levels, chans)),
            dma((levels, chans)),
        ],
        compiler_params=pltpu.CompilerParams(has_side_effects=True, vmem_limit_bytes=63 * 1024 * 1024),
    )(legendre, outgoing, mixing)
    return arrived


def body(chans, lats, grid_in, quad_weights, legendre, mixing):
    groups, rows_lat, length = grid_in.shape
    orders = legendre.shape[0]
    degrees = mixing.shape[1]
    chunks = chunks_of(orders, chans)
    fits = (
        chunks > 0
        and chans > 1
        and chans & (chans - 1) == 0
        and 2 * groups == LANES
        and rows_lat % 16 == 0
        and degrees % 16 == 0
        and orders * lats == M
        and degrees * lats == legendre.shape[1]
        and lats * (orders // (chunks * chans)) % 8 == 0
    )
    if not fits:
        return general(chans, grid_in, quad_weights, legendre, mixing)
    fourier = fourier_table(M, length)
    spectra = jnp.einsum("ctn,rmn->mtrc", grid_in, fourier, preferred_element_type=jnp.float32)
    spectra = spectra * quad_weights[None, :, None, None]
    weighted = spectra.astype(jnp.bfloat16).reshape(lats, orders, rows_lat, 2 * groups)
    gridded = exchange(chans, chunks, legendre, weighted, mixing)
    spread = gridded.reshape(M, rows_lat, 2, groups)
    restored = jnp.einsum("mtrc,rmn->ctn", spread, fourier, preferred_element_type=jnp.float32)
    return (restored + grid_in.astype(jnp.float32)).astype(jnp.bfloat16)


def solution(mesh):
    return jax.shard_map(
        functools.partial(body, mesh.shape["chan"], mesh.shape["lat"]),
        mesh=mesh,
        in_specs=(
            P("chan", "lat", None),
            P("lat"),
            P("lat", None, None),
            P(None, "lat", "chan", None),
        ),
        out_specs=P("chan", "lat", None),
        check_vma=False,
    )
```

```python
import functools
import math

import jax
import jax.numpy as jnp
import numpy as np
from jax import lax
from jax.experimental import pallas as pl
from jax.experimental.pallas import tpu as pltpu
from jax.sharding import PartitionSpec as P

M = 384
PIECES = (2, 1)


def fourier_table(number, length):
    orders = jnp.arange(number, dtype=jnp.int32)
    points = jnp.arange(length, dtype=jnp.int32)
    phases = orders[:, None] * points[None, :] % length
    angles = phases.astype(jnp.float32) * (2.0 * math.pi / length)
    factor = 1.0 / math.sqrt(length)
    return jnp.stack([jnp.cos(angles) * factor, -jnp.sin(angles) * factor]).astype(jnp.bfloat16)


def step_of(part):
    return next(count for count in (4, 3, 2, 1) if part % count == 0)


def price(legendre, columns):
    orders, degrees, points = legendre.shape
    return pl.CostEstimate(
        flops=2 * orders * degrees * points * columns,
        bytes_accessed=2 * orders * (degrees * points + (degrees + points) * columns),
        transcendentals=0,
    )


def analyse(legendre, gathered, chans):
    lats, orders, rows_lat, columns = gathered.shape
    degrees = legendre.shape[1] // lats
    part = orders // chans
    step = step_of(part)
    runs = part // step

    def kernel(table_ref, values_ref, out_ref):
        for at in range(step):
            values = values_ref[:, at].reshape(lats * rows_lat, columns)
            sums = jnp.dot(table_ref[at], values, preferred_element_type=jnp.float32)
            out_ref[:, 0, at] = sums.astype(jnp.bfloat16).reshape(lats, degrees, columns)

    return pl.pallas_call(
        kernel,
        grid=(orders // step,),
        in_specs=[
            pl.BlockSpec((step,) + legendre.shape[1:], lambda g: (g, 0, 0)),
            pl.BlockSpec((lats, step, rows_lat, columns), lambda g: (0, g, 0, 0)),
        ],
        out_specs=pl.BlockSpec(
            (lats, 1, step, degrees, columns), lambda g: (0, g // runs, g % runs, 0, 0)
        ),
        out_shape=jax.ShapeDtypeStruct((lats, chans, part, degrees, columns), jnp.bfloat16),
        cost_estimate=price(legendre, columns),
    )(legendre, gathered)


def synthesise(legendre, returned, rows_lat):
    lats, chans, part, degrees, columns = returned.shape
    orders = legendre.shape[0]
    step = step_of(part)
    runs = part // step

    def kernel(table_ref, values_ref, out_ref):
        for at in range(step):
            values = values_ref[:, 0, at].reshape(lats * degrees, columns)
            sums = lax.dot_general(
                table_ref[at],
                values,
                (((0,), (0,)), ((), ())),
                preferred_element_type=jnp.float32,
            )
            out_ref[:, at] = sums.astype(jnp.bfloat16).reshape(lats, rows_lat, columns)

    return pl.pallas_call(
        kernel,
        grid=(orders // step,),
        in_specs=[
            pl.BlockSpec((step,) + legendre.shape[1:], lambda g: (g, 0, 0)),
            pl.BlockSpec(
                (lats, 1, step, degrees, columns), lambda g: (0, g // runs, g % runs, 0, 0)
            ),
        ],
        out_specs=pl.BlockSpec((lats, step, rows_lat, columns), lambda g: (0, g, 0, 0)),
        out_shape=jax.ShapeDtypeStruct((lats, orders, rows_lat, columns), jnp.bfloat16),
        cost_estimate=price(legendre, columns),
    )(legendre, returned)


def general(chans, grid_in, quad_weights, legendre, mixing):
    groups = grid_in.shape[0]
    rows_lat = grid_in.shape[1]
    length = grid_in.shape[2]
    orders = legendre.shape[0]
    degrees = mixing.shape[1]
    lats = legendre.shape[1] // degrees
    part = -(-orders // chans)
    padding = part * chans - orders
    everyone = ("lat", "chan")

    channel = jnp.arange(chans * groups)
    place = channel // groups * (2 * groups) + channel % groups
    column = jnp.arange(2 * chans * groups)
    to_real = (column == place[:, None]).astype(jnp.bfloat16)
    to_imag = (column == place[:, None] + groups).astype(jnp.bfloat16)

    def spread_out(table):
        return jnp.einsum(
            "rlcd,rdy->lcy", mixing, table, preferred_element_type=jnp.float32
        ).astype(jnp.bfloat16)

    blocks = jnp.concatenate(
        [
            spread_out(jnp.stack([to_real, to_imag])),
            spread_out(jnp.stack([to_imag, -to_real])),
        ],
        axis=1,
    )
    weights = lax.all_gather(blocks, "chan", axis=0)
    fourier = fourier_table(M, length)
    spectra = jnp.einsum("ctn,rmn->mtrc", grid_in, fourier, preferred_element_type=jnp.float32)
    spectra = spectra * quad_weights[None, :, None, None]
    weighted = spectra.astype(jnp.bfloat16).reshape(M, rows_lat, 2 * groups)
    gathered = lax.all_to_all(weighted, "lat", split_axis=0, concat_axis=0, tiled=True)
    gathered = gathered.reshape(lats, orders, rows_lat, 2 * groups)
    fits = padding == 0 and rows_lat % 16 == 0 and degrees % 16 == 0
    if fits:
        outgoing = analyse(legendre, gathered, chans)
    else:
        whole = gathered.transpose(1, 0, 2, 3).reshape(orders, lats * rows_lat, 2 * groups)
        coeffs = jnp.einsum(
            "mlt,mtk->mlk", legendre, whole, preferred_element_type=jnp.float32
        ).astype(jnp.bfloat16)
        coeffs = jnp.pad(coeffs, ((0, padding), (0, 0), (0, 0)))
        outgoing = coeffs.reshape(chans, part, lats, degrees, 2 * groups)
        outgoing = outgoing.transpose(2, 0, 1, 3, 4)
    pieces = next(count for count in PIECES if part % count == 0)
    width = part // pieces
    place_lat = lax.axis_index("lat")
    peers = jnp.arange(lats).reshape(lats, 1, 1, 1, 1)

    def exchange(buffer, axes):
        flat = buffer.reshape((-1,) + buffer.shape[-3:])
        flat = lax.all_to_all(flat, axes, split_axis=0, concat_axis=0, tiled=True)
        return flat.reshape(buffer.shape)

    def mix(arrived):
        mixed = jnp.einsum(
            "ikmlx,klxy->limy", arrived, weights, preferred_element_type=jnp.float32
        ).astype(jnp.bfloat16)
        mixed = mixed.reshape(degrees, lats, width, chans, 2 * groups)
        return mixed.transpose(1, 3, 2, 0, 4)

    received = [exchange(outgoing[:, :, :width], ("lat", "chan"))]
    own = []
    for piece in range(1, pieces + 1):
        mixed = mix(received[-1])
        if piece < pieces:
            own.append(lax.dynamic_index_in_dim(mixed, place_lat, 0, keepdims=False))
            coming = outgoing[:, :, piece * width : (piece + 1) * width]
            mixed = jnp.where(peers >= place_lat, coming, mixed)
        received.append(exchange(mixed, ("lat", "chan")))
    if own:
        own = exchange(jnp.concatenate(own, axis=1), "chan")
    returned = []
    for piece in range(pieces):
        block = received[piece + 1]
        if piece < pieces - 1:
            mine = own[None, :, piece * width : (piece + 1) * width]
            block = jnp.where(peers == place_lat, mine, block)
        returned.append(jnp.where(peers >= place_lat, block, jnp.zeros_like(block)))
    returned = jnp.concatenate(returned, axis=2)
    if fits:
        synthesis = synthesise(legendre, returned, rows_lat)
    else:
        mixed_coef = returned.transpose(1, 2, 0, 3, 4)
        mixed_coef = mixed_coef.reshape(chans * part, lats * degrees, 2 * groups)[:orders]
        synthesis = jnp.einsum(
            "mlt,mlk->mtk", legendre, mixed_coef, preferred_element_type=jnp.float32
        ).astype(jnp.bfloat16)
        synthesis = synthesis.reshape(orders, lats, rows_lat, 2 * groups).transpose(1, 0, 2, 3)
    synthesis = synthesis.reshape(lats * orders, rows_lat, 2 * groups)
    gridded = lax.all_to_all(synthesis, "lat", split_axis=0, concat_axis=0, tiled=True)
    spread = gridded.reshape(M, rows_lat, 2, groups)
    restored = jnp.einsum("mtrc,rmn->ctn", spread, fourier, preferred_element_type=jnp.float32)
    return (restored + grid_in.astype(jnp.float32)).astype(jnp.bfloat16)


MESH = pl.DeviceIdType.MESH
LANES = 128
TILE = 16
VMEM_LIMIT = 67043328


def chunks_of(orders, chans):
    return next((count for count in (4, 3, 2, 1) if orders % (count * chans) == 0), 0)


def exchange_kernel(
    lats, chans, chunks,
    leg, grid, table, quad, mix, arrived, weights,
    field, turned, waves, w_send, w_recv, c_send, c_recv, x_send, x_recv, s_send,
    legs, tiles, wide,
    leg_sem, tile_sem, own_sem, field_sem,
    ws_sem, wr_sem, cs_sem, cr_sem, xs_sem, xr_sem, ss_sem, sr_sem, gs_sem, gr_sem,
):
    here = lax.axis_index("lat")
    group = lax.axis_index("chan")
    orders, degrees_all, points_all = leg.shape
    degrees = degrees_all // lats
    points = points_all // lats
    size = orders // chunks
    part = size // chans
    rows = lats * part
    columns = w_send.shape[-1]
    groups, _, length = field.shape
    half = columns // 2
    folds = length // columns
    every = lats * size
    span = tiles.shape[1]
    bands = degrees // span
    inner = tiles.shape[3] // chans
    depth = rows * degrees
    batch = 256 // groups

    def to(lat, chan):
        return {"device_id": {"lat": lat, "chan": chan}, "device_id_type": MESH}

    def each_peer(do):
        def step(d, carry):
            do(lax.rem(here + d, lats))
            return carry

        lax.fori_loop(1, lats, step, 0)

    def each_pair(low, high, do):
        def step(n, carry):
            lat = n // chans
            chan = n % chans

            @pl.when(jnp.logical_or(lat != here, chan != group))
            def _():
                do(lat, chan)

            return carry

        lax.fori_loop(low * chans, high * chans, step, 0)

    def weighted_copy(j, peer, source):
        at = pl.ds(j * size, size)
        return pltpu.make_async_remote_copy(
            src_ref=w_send.at[peer, at], dst_ref=w_recv.at[source, at],
            send_sem=ws_sem.at[j, peer], recv_sem=wr_sem.at[j, source],
            **to(peer, group),
        )

    def send_weighted(j):
        each_peer(lambda peer: weighted_copy(j, peer, here).start())

    def lane_of(count):
        return lax.broadcasted_iota(jnp.int32, (count, columns), 1) < half

    def field_copy(block):
        at = pl.ds(block * TILE, TILE)
        return pltpu.make_async_copy(grid.at[:, at], field.at[:, at], field_sem.at[block])

    def turn(block):
        count = groups * TILE

        def widen(c, carry):
            values = field[c, pl.ds(block * TILE, TILE), :].astype(jnp.float32)
            for n in range(folds):
                wide[pl.ds(n * count + c * TILE, TILE), :] = values[:, n * columns : (n + 1) * columns]
            return carry

        lax.fori_loop(0, groups, widen, 0)

        def pick(t, carry):
            for n in range(folds):
                values = wide[pl.ds(n * count + t, groups, stride=TILE), :]
                turned[block * TILE + t, :, pl.ds(n * columns, columns)] = values.astype(jnp.bfloat16)
            return carry

        lax.fori_loop(0, TILE, pick, 0)

    def transform(j, send):
        lane = lane_of(every)
        at = pl.ds(j * every, every)
        lines = pl.ds(j * size, size)

        def step(b, carry):
            first = b * batch
            left = jnp.concatenate([waves[0, at], waves[1, at]], axis=0)
            right = turned[pl.ds(first, batch)].reshape(batch * groups, length)
            sums = lax.dot_general(left, right, (((1,), (1,)), ((), ())), preferred_element_type=jnp.float32)
            for pair in range(batch // 2):
                cut = slice(pair * columns, (pair + 1) * columns)
                real, imag = sums[:every, cut], sums[every:, cut]
                t = first + 2 * pair
                even = jnp.where(lane, real, pltpu.roll(imag, half, 1)) * quad[t]
                odd = jnp.where(lane, pltpu.roll(real, half, 1), imag) * quad[t + 1]
                wide[pl.ds(t, every, stride=points), :] = even
                wide[pl.ds(t + 1, every, stride=points), :] = odd
            return carry

        lax.fori_loop(0, points // batch, step, 0)

        def fold(d, carry):
            peer = lax.rem(here + d, lats)
            values = wide[pl.ds(peer * size * points, size * points), :].astype(jnp.bfloat16)
            w_send[peer, lines] = values.reshape(size, points, columns)

            @pl.when(d > 0)
            def _():
                if send:
                    weighted_copy(j, peer, here).start()

            return carry

        lax.fori_loop(0, lats, fold, 0)
        w_recv[here, lines] = w_send[here, lines]

    def coeff_copy(j, lat, chan, from_lat, from_chan):
        at = pl.ds(j * part, part)
        return pltpu.make_async_remote_copy(
            src_ref=c_send.at[lat, chan, at], dst_ref=c_recv.at[from_lat, from_chan, at],
            send_sem=cs_sem.at[j, lat, chan], recv_sem=cr_sem.at[j, from_lat, from_chan],
            **to(lat, chan),
        )

    def mixed_copy(j, lat, chan, from_lat, from_chan):
        at = pl.ds(j * part, part)
        return pltpu.make_async_remote_copy(
            src_ref=x_send.at[lat, chan, at], dst_ref=x_recv.at[from_lat, from_chan, at],
            send_sem=xs_sem.at[j, lat, chan], recv_sem=xr_sem.at[j, from_lat, from_chan],
            **to(lat, chan),
        )

    def synthesis_copy(j, peer, source):
        at = pl.ds(j * size, size)
        return pltpu.make_async_remote_copy(
            src_ref=s_send.at[peer, at], dst_ref=arrived.at[source, at],
            send_sem=ss_sem.at[j, peer], recv_sem=sr_sem.at[j, source],
            **to(peer, group),
        )

    def own_synthesis(j):
        at = pl.ds(j * size, size)
        return pltpu.make_async_copy(s_send.at[here, at], arrived.at[here, at], own_sem.at[1])

    def leg_copy(use, j):
        return pltpu.make_async_copy(leg.at[pl.ds(j * size, size)], legs.at[use % 2], leg_sem.at[use % 2])

    def analyse(use, j):
        def step(n, carry):
            at = j * size + n
            values = w_recv[:, at].reshape(lats * points, columns)
            sums = jnp.dot(legs[use % 2, n], values, preferred_element_type=jnp.float32)
            c_send[:, n // part, j * part + n % part] = sums.astype(jnp.bfloat16).reshape(lats, degrees, columns)
            return carry

        lax.fori_loop(0, size, step, 0)
        at = pl.ds(j * part, part)
        each_pair(here, lats, lambda lat, chan: coeff_copy(j, lat, chan, here, group).start())
        c_recv[here, group, at] = c_send[here, group, at]

    def synthesise(use, j):
        def step(n, carry):
            values = x_recv[:, n // part, j * part + n % part].reshape(lats * degrees, columns)
            sums = lax.dot_general(
                legs[use % 2, n], values, (((0,), (0,)), ((), ())), preferred_element_type=jnp.float32
            )
            s_send[:, j * size + n] = sums.astype(jnp.bfloat16).reshape(lats, points, columns)
            return carry

        lax.fori_loop(0, size, step, 0)
        each_peer(lambda peer: synthesis_copy(j, peer, here).start())
        own_synthesis(j).start()
        own_synthesis(j).wait()

    def tile_copies(band, slot, do):
        at = pl.ds(band * span, span)
        for chan in range(chans):
            for r in range(2):
                target = tiles.at[slot, :, r, pl.ds(chan * inner, inner)]
                sem = tile_sem.at[slot, chan, r]

                @pl.when(chan == group)
                def _():
                    do(pltpu.make_async_copy(mix.at[r, at], target, sem))

                @pl.when(chan != group)
                def _():
                    do(pltpu.make_async_copy(weights.at[chan, r, at], target, sem))

    def mix_chunk(j):
        at = pl.ds(j * part, part)
        block = part * degrees
        tile_copies(0, 0, lambda copy: copy.start())

        def widen(s, carry):
            for chan in range(chans):
                values = c_recv[s, chan, at].astype(jnp.float32)
                wide[pl.ds(chan * depth + s * block, block), :] = values.reshape(block, columns)
            return carry

        lax.fori_loop(0, lats, widen, 0)
        lane = lane_of(rows)
        after = chans * depth

        def band_step(band, carry):
            slot = band % 2

            @pl.when(band + 1 < bands)
            def _():
                tile_copies(band + 1, 1 - slot, lambda copy: copy.start())

            tile_copies(band, slot, lambda copy: copy.wait())

            def degree_step(n, carry):
                line = band * span + n
                taken = [wide[pl.ds(chan * depth + line, rows, stride=degrees), :] for chan in range(chans)]
                real, imag = [], []
                for low, high in zip(taken[0::2], taken[1::2]):
                    real.append(jnp.where(lane, low, pltpu.roll(high, half, 1)))
                    imag.append(jnp.where(lane, pltpu.roll(low, half, 1), high))
                stacked = jnp.concatenate(
                    [jnp.concatenate(real, axis=1), jnp.concatenate(imag, axis=1)], axis=0
                ).astype(jnp.bfloat16)
                by_real = jnp.dot(stacked, tiles[slot, n, 0], preferred_element_type=jnp.float32)
                by_imag = jnp.dot(stacked, tiles[slot, n, 1], preferred_element_type=jnp.float32)
                real_out = by_real[:rows] - by_imag[rows:]
                imag_out = by_real[rows:] + by_imag[:rows]
                for pair in range(chans // 2):
                    first = real_out[:, pair * columns : (pair + 1) * columns]
                    second = imag_out[:, pair * columns : (pair + 1) * columns]
                    start = after + 2 * pair * depth + line
                    even = jnp.where(lane, first, pltpu.roll(second, half, 1))
                    odd = jnp.where(lane, pltpu.roll(first, half, 1), second)
                    wide[pl.ds(start, rows, stride=degrees), :] = even
                    wide[pl.ds(start + depth, rows, stride=degrees), :] = odd
                return carry

            lax.fori_loop(0, span, degree_step, 0)
            return carry

        lax.fori_loop(0, bands, band_step, 0)

        def narrow(s, carry):
            for chan in range(chans):
                values = wide[pl.ds(after + chan * depth + s * block, block), :].astype(jnp.bfloat16)
                x_send[s, chan, at] = values.reshape(part, degrees, columns)
            return carry

        lax.fori_loop(0, here + 1, narrow, 0)
        each_pair(0, here + 1, lambda lat, chan: mixed_copy(j, lat, chan, here, group).start())
        x_recv[here, group, at] = x_send[here, group, at]

    steps = []
    distance = chans // 2
    held = 1
    while distance:
        steps.append(distance)
        distance //= 2

    def gather_copies(level):
        distance = steps[level]
        peer = jnp.bitwise_xor(group, distance)
        copies = []
        for n in range(2**level):
            offset = sum(steps[b] for b in range(level) if n >> b & 1)
            shard = jnp.bitwise_xor(group, offset)
            source = mix if offset == 0 else weights.at[shard]
            copies.append(
                pltpu.make_async_remote_copy(
                    src_ref=source, dst_ref=weights.at[shard],
                    send_sem=gs_sem.at[level, n], recv_sem=gr_sem.at[level, n],
                    **to(here, peer),
                )
            )
        return copies

    use = 0
    order = []
    plan = []
    for j in range(chunks):
        plan.append(("L", j))
        if j >= 1:
            plan.append(("X", j - 1))
        if j >= 2:
            plan.append(("S", j - 2))
    plan.append(("X", chunks - 1))
    if chunks >= 2:
        plan.append(("S", chunks - 2))
    plan.append(("S", chunks - 1))
    order = [(kind, j) for kind, j in plan if kind != "X"]

    table_copy = pltpu.make_async_copy(table, waves, own_sem.at[0])
    blocks = points // TILE
    field_copy(0).start()
    table_copy.start()
    for block in range(1, blocks):
        field_copy(block).start()
    leg_copy(0, order[0][1]).start()
    for copy in gather_copies(0):
        copy.start()
    for block in range(blocks):
        field_copy(block).wait()
        turn(block)
    table_copy.wait()
    for j in range(chunks):
        transform(j, j < 2)

    def clear(s, carry):
        x_recv[s] = jnp.zeros(x_recv.shape[1:], x_recv.dtype)
        return carry

    lax.fori_loop(0, here, clear, 0)

    use = 0
    gathered = False
    for kind, j in plan:
        if kind == "X":
            if not gathered:
                for level in range(len(steps)):
                    for copy in gather_copies(level):
                        copy.wait_recv()
                    if level + 1 < len(steps):
                        for copy in gather_copies(level + 1):
                            copy.start()
                gathered = True
            each_pair(0, here + 1, lambda lat, chan: coeff_copy(j, here, group, lat, chan).wait_recv())
            mix_chunk(j)
            continue
        if use + 1 < len(order):
            leg_copy(use + 1, order[use + 1][1]).start()
        if kind == "L":
            each_peer(lambda peer: weighted_copy(j, here, peer).wait_recv())
            leg_copy(use, j).wait()
            analyse(use, j)
            if j + 2 < chunks:
                send_weighted(j + 2)
        else:
            each_pair(here, lats, lambda lat, chan: mixed_copy(j, here, group, lat, chan).wait_recv())
            leg_copy(use, j).wait()
            synthesise(use, j)
        use += 1

    for level in range(len(steps)):
        for copy in gather_copies(level):
            copy.wait_send()
    for j in range(chunks):
        each_peer(lambda peer: weighted_copy(j, peer, here).wait_send())
        each_pair(here, lats, lambda lat, chan: coeff_copy(j, lat, chan, here, group).wait_send())
        each_pair(0, here + 1, lambda lat, chan: mixed_copy(j, lat, chan, here, group).wait_send())
    for j in range(chunks):
        each_peer(lambda peer: synthesis_copy(j, here, peer).wait_recv())
        each_peer(lambda peer: synthesis_copy(j, peer, here).wait_send())


def exchange(chans, lats, chunks, legendre, grid_in, table, quad_weights, mixing):
    orders = legendre.shape[0]
    groups, points, length = grid_in.shape
    degrees = mixing.shape[1]
    columns = 2 * groups
    size = orders // chunks
    part = size // chans
    rows = lats * part
    span = next(count for count in (8, 6, 4, 3, 2, 1) if degrees % count == 0)
    inner = mixing.shape[2]
    levels = max(1, chans.bit_length() - 1)
    spectral = (lats, chans, orders // chans, degrees, columns)
    gridded = (lats, orders, points, columns)
    scratch = max(2 * chans * rows * degrees, lats * size * points, length // columns * groups * TILE)
    half = jnp.bfloat16
    dma = pltpu.SemaphoreType.DMA
    anywhere = pl.BlockSpec(memory_space=pl.ANY)
    arrived, _ = pl.pallas_call(
        functools.partial(exchange_kernel, lats, chans, chunks),
        in_specs=[anywhere, anywhere, anywhere, pl.BlockSpec(memory_space=pltpu.SMEM), anywhere],
        out_specs=[anywhere] * 2,
        out_shape=[
            jax.ShapeDtypeStruct(gridded, half),
            jax.ShapeDtypeStruct((chans,) + mixing.shape, half),
        ],
        scratch_shapes=[
            pltpu.VMEM(grid_in.shape, half),
            pltpu.VMEM((points, groups, length), half),
            pltpu.VMEM(table.shape, half),
            pltpu.VMEM(gridded, half),
            pltpu.VMEM(gridded, half),
            pltpu.VMEM(spectral, half),
            pltpu.VMEM(spectral, half),
            pltpu.VMEM(spectral, half),
            pltpu.VMEM(spectral, half),
            pltpu.VMEM(gridded, half),
            pltpu.VMEM((2, size) + legendre.shape[1:], half),
            pltpu.VMEM((2, span, 2, chans * inner, mixing.shape[3]), half),
            pltpu.VMEM((scratch, columns), jnp.float32),
            dma((2,)),
            dma((2, chans, 2)),
            dma((2,)),
            dma((points // TILE,)),
            dma((chunks, lats)),
            dma((chunks, lats)),
            dma((chunks, lats, chans)),
            dma((chunks, lats, chans)),
            dma((chunks, lats, chans)),
            dma((chunks, lats, chans)),
            dma((chunks, lats)),
            dma((chunks, lats)),
            dma((levels, chans)),
            dma((levels, chans)),
        ],
        compiler_params=pltpu.CompilerParams(has_side_effects=True, vmem_limit_bytes=VMEM_LIMIT),
    )(legendre, grid_in, table, quad_weights, mixing)
    return arrived


def restore_kernel(chunks, spectra, grid, waves, out, lines, sums):
    lats, orders, tile, columns = spectra.shape
    groups, _, length = grid.shape
    size = orders // chunks
    total = lats * orders
    half = columns // 2
    folds = length // columns
    batch = 256 // groups
    count = groups * tile
    lane = lax.broadcasted_iota(jnp.int32, (total, columns), 1) < half

    def widen(lat, carry):
        for chunk in range(chunks):
            values = spectra[lat, pl.ds(chunk * size, size)].astype(jnp.float32)
            start = (chunk * lats + lat) * size * tile
            lines[pl.ds(start, size * tile), :] = values.reshape(size * tile, columns)
        return carry

    lax.fori_loop(0, lats, widen, 0)

    def step(b, carry):
        first = b * batch
        real, imag = [], []
        for pair in range(batch // 2):
            t = first + 2 * pair
            low = lines[pl.ds(t, total, stride=tile), :]
            high = lines[pl.ds(t + 1, total, stride=tile), :]
            real.append(jnp.where(lane, low, pltpu.roll(high, half, 1)))
            imag.append(jnp.where(lane, pltpu.roll(low, half, 1), high))
        left = jnp.concatenate([jnp.concatenate(real, axis=1), jnp.concatenate(imag, axis=1)], axis=0)
        result = lax.dot_general(
            left.astype(jnp.bfloat16), waves[...].reshape(2 * total, length),
            (((0,), (0,)), ((), ())), preferred_element_type=jnp.float32,
        )
        for t in range(batch):
            for n in range(folds):
                values = result[t * groups : (t + 1) * groups, n * columns : (n + 1) * columns]
                sums[pl.ds(n * count + first + t, groups, stride=tile), :] = values
        return carry

    lax.fori_loop(0, tile // batch, step, 0)

    def add(c, carry):
        for n in range(folds):
            cut = pl.ds(n * columns, columns)
            values = sums[pl.ds(n * count + c * tile, tile), :] + grid[c, :, cut].astype(jnp.float32)
            out[c, :, cut] = values.astype(jnp.bfloat16)
        return carry

    lax.fori_loop(0, groups, add, 0)


def restore(chunks, gridded, grid_in, table):
    lats, orders, points, columns = gridded.shape
    groups, _, length = grid_in.shape
    by_rows = pl.BlockSpec((groups, TILE, length), lambda g: (0, g, 0))
    return pl.pallas_call(
        functools.partial(restore_kernel, chunks),
        grid=(points // TILE,),
        in_specs=[
            pl.BlockSpec((lats, orders, TILE, columns), lambda g: (0, 0, g, 0)),
            by_rows,
            pl.BlockSpec(table.shape, lambda g: (0, 0, 0)),
        ],
        out_specs=by_rows,
        out_shape=jax.ShapeDtypeStruct(grid_in.shape, jnp.bfloat16),
        scratch_shapes=[
            pltpu.VMEM((lats * orders * TILE, columns), jnp.float32),
            pltpu.VMEM((length // columns * groups * TILE, columns), jnp.float32),
        ],
        compiler_params=pltpu.CompilerParams(vmem_limit_bytes=VMEM_LIMIT),
    )(gridded, grid_in, table)


def wave_table(lats, orders, chunks, length):
    at = np.arange(lats * orders).reshape(lats, chunks, orders // chunks)
    phases = at.transpose(1, 0, 2).reshape(-1, 1) * np.arange(length)[None, :] % length
    angles = phases.astype(np.float32) * np.float32(2.0 * math.pi / length)
    values = np.stack([np.cos(angles), -np.sin(angles)]) * np.float32(1.0 / math.sqrt(length))
    return jnp.asarray(values.astype(jnp.bfloat16))


def body(chans, lats, grid_in, quad_weights, legendre, mixing):
    groups, rows_lat, length = grid_in.shape
    orders = legendre.shape[0]
    degrees = mixing.shape[1]
    chunks = chunks_of(orders, chans)
    fits = (
        chunks > 0
        and chans > 1
        and chans & (chans - 1) == 0
        and 2 * groups == LANES
        and rows_lat % TILE == 0
        and length % LANES == 0
        and degrees % TILE == 0
        and orders * lats == M
        and degrees * lats == legendre.shape[1]
        and lats * (orders // (chunks * chans)) % 8 == 0
    )
    if not fits:
        return general(chans, grid_in, quad_weights, legendre, mixing)
    table = wave_table(lats, orders, chunks, length)
    gridded = exchange(chans, lats, chunks, legendre, grid_in, table, quad_weights, mixing)
    return restore(chunks, gridded, grid_in, table)


def solution(mesh):
    return jax.shard_map(
        functools.partial(body, mesh.shape["chan"], mesh.shape["lat"]),
        mesh=mesh,
        in_specs=(
            P("chan", "lat", None),
            P("lat"),
            P("lat", None, None),
            P(None, "lat", "chan", None),
        ),
        out_specs=P("chan", "lat", None),
        check_vma=False,
    )
```

```python
import functools
import math

import jax
import jax.numpy as jnp
import numpy as np
from jax import lax
from jax.experimental import pallas as pl
from jax.experimental.pallas import tpu as pltpu
from jax.sharding import PartitionSpec as P

M = 384
PIECES = (2, 1)


def fourier_table(number, length):
    orders = jnp.arange(number, dtype=jnp.int32)
    points = jnp.arange(length, dtype=jnp.int32)
    phases = orders[:, None] * points[None, :] % length
    angles = phases.astype(jnp.float32) * (2.0 * math.pi / length)
    factor = 1.0 / math.sqrt(length)
    return jnp.stack([jnp.cos(angles) * factor, -jnp.sin(angles) * factor]).astype(jnp.bfloat16)


def step_of(part):
    return next(count for count in (4, 3, 2, 1) if part % count == 0)


def price(legendre, columns):
    orders, degrees, points = legendre.shape
    return pl.CostEstimate(
        flops=2 * orders * degrees * points * columns,
        bytes_accessed=2 * orders * (degrees * points + (degrees + points) * columns),
        transcendentals=0,
    )


def analyse(legendre, gathered, chans):
    lats, orders, rows_lat, columns = gathered.shape
    degrees = legendre.shape[1] // lats
    part = orders // chans
    step = step_of(part)
    runs = part // step

    def kernel(table_ref, values_ref, out_ref):
        for at in range(step):
            values = values_ref[:, at].reshape(lats * rows_lat, columns)
            sums = jnp.dot(table_ref[at], values, preferred_element_type=jnp.float32)
            out_ref[:, 0, at] = sums.astype(jnp.bfloat16).reshape(lats, degrees, columns)

    return pl.pallas_call(
        kernel,
        grid=(orders // step,),
        in_specs=[
            pl.BlockSpec((step,) + legendre.shape[1:], lambda g: (g, 0, 0)),
            pl.BlockSpec((lats, step, rows_lat, columns), lambda g: (0, g, 0, 0)),
        ],
        out_specs=pl.BlockSpec(
            (lats, 1, step, degrees, columns), lambda g: (0, g // runs, g % runs, 0, 0)
        ),
        out_shape=jax.ShapeDtypeStruct((lats, chans, part, degrees, columns), jnp.bfloat16),
        cost_estimate=price(legendre, columns),
    )(legendre, gathered)


def synthesise(legendre, returned, rows_lat):
    lats, chans, part, degrees, columns = returned.shape
    orders = legendre.shape[0]
    step = step_of(part)
    runs = part // step

    def kernel(table_ref, values_ref, out_ref):
        for at in range(step):
            values = values_ref[:, 0, at].reshape(lats * degrees, columns)
            sums = lax.dot_general(
                table_ref[at],
                values,
                (((0,), (0,)), ((), ())),
                preferred_element_type=jnp.float32,
            )
            out_ref[:, at] = sums.astype(jnp.bfloat16).reshape(lats, rows_lat, columns)

    return pl.pallas_call(
        kernel,
        grid=(orders // step,),
        in_specs=[
            pl.BlockSpec((step,) + legendre.shape[1:], lambda g: (g, 0, 0)),
            pl.BlockSpec(
                (lats, 1, step, degrees, columns), lambda g: (0, g // runs, g % runs, 0, 0)
            ),
        ],
        out_specs=pl.BlockSpec((lats, step, rows_lat, columns), lambda g: (0, g, 0, 0)),
        out_shape=jax.ShapeDtypeStruct((lats, orders, rows_lat, columns), jnp.bfloat16),
        cost_estimate=price(legendre, columns),
    )(legendre, returned)


def general(chans, grid_in, quad_weights, legendre, mixing):
    groups = grid_in.shape[0]
    rows_lat = grid_in.shape[1]
    length = grid_in.shape[2]
    orders = legendre.shape[0]
    degrees = mixing.shape[1]
    lats = legendre.shape[1] // degrees
    part = -(-orders // chans)
    padding = part * chans - orders
    everyone = ("lat", "chan")

    channel = jnp.arange(chans * groups)
    place = channel // groups * (2 * groups) + channel % groups
    column = jnp.arange(2 * chans * groups)
    to_real = (column == place[:, None]).astype(jnp.bfloat16)
    to_imag = (column == place[:, None] + groups).astype(jnp.bfloat16)

    def spread_out(table):
        return jnp.einsum(
            "rlcd,rdy->lcy", mixing, table, preferred_element_type=jnp.float32
        ).astype(jnp.bfloat16)

    blocks = jnp.concatenate(
        [
            spread_out(jnp.stack([to_real, to_imag])),
            spread_out(jnp.stack([to_imag, -to_real])),
        ],
        axis=1,
    )
    weights = lax.all_gather(blocks, "chan", axis=0)
    fourier = fourier_table(M, length)
    spectra = jnp.einsum("ctn,rmn->mtrc", grid_in, fourier, preferred_element_type=jnp.float32)
    spectra = spectra * quad_weights[None, :, None, None]
    weighted = spectra.astype(jnp.bfloat16).reshape(M, rows_lat, 2 * groups)
    gathered = lax.all_to_all(weighted, "lat", split_axis=0, concat_axis=0, tiled=True)
    gathered = gathered.reshape(lats, orders, rows_lat, 2 * groups)
    fits = padding == 0 and rows_lat % 16 == 0 and degrees % 16 == 0
    if fits:
        outgoing = analyse(legendre, gathered, chans)
    else:
        whole = gathered.transpose(1, 0, 2, 3).reshape(orders, lats * rows_lat, 2 * groups)
        coeffs = jnp.einsum(
            "mlt,mtk->mlk", legendre, whole, preferred_element_type=jnp.float32
        ).astype(jnp.bfloat16)
        coeffs = jnp.pad(coeffs, ((0, padding), (0, 0), (0, 0)))
        outgoing = coeffs.reshape(chans, part, lats, degrees, 2 * groups)
        outgoing = outgoing.transpose(2, 0, 1, 3, 4)
    pieces = next(count for count in PIECES if part % count == 0)
    width = part // pieces
    place_lat = lax.axis_index("lat")
    peers = jnp.arange(lats).reshape(lats, 1, 1, 1, 1)

    def exchange(buffer, axes):
        flat = buffer.reshape((-1,) + buffer.shape[-3:])
        flat = lax.all_to_all(flat, axes, split_axis=0, concat_axis=0, tiled=True)
        return flat.reshape(buffer.shape)

    def mix(arrived):
        mixed = jnp.einsum(
            "ikmlx,klxy->limy", arrived, weights, preferred_element_type=jnp.float32
        ).astype(jnp.bfloat16)
        mixed = mixed.reshape(degrees, lats, width, chans, 2 * groups)
        return mixed.transpose(1, 3, 2, 0, 4)

    received = [exchange(outgoing[:, :, :width], ("lat", "chan"))]
    own = []
    for piece in range(1, pieces + 1):
        mixed = mix(received[-1])
        if piece < pieces:
            own.append(lax.dynamic_index_in_dim(mixed, place_lat, 0, keepdims=False))
            coming = outgoing[:, :, piece * width : (piece + 1) * width]
            mixed = jnp.where(peers >= place_lat, coming, mixed)
        received.append(exchange(mixed, ("lat", "chan")))
    if own:
        own = exchange(jnp.concatenate(own, axis=1), "chan")
    returned = []
    for piece in range(pieces):
        block = received[piece + 1]
        if piece < pieces - 1:
            mine = own[None, :, piece * width : (piece + 1) * width]
            block = jnp.where(peers == place_lat, mine, block)
        returned.append(jnp.where(peers >= place_lat, block, jnp.zeros_like(block)))
    returned = jnp.concatenate(returned, axis=2)
    if fits:
        synthesis = synthesise(legendre, returned, rows_lat)
    else:
        mixed_coef = returned.transpose(1, 2, 0, 3, 4)
        mixed_coef = mixed_coef.reshape(chans * part, lats * degrees, 2 * groups)[:orders]
        synthesis = jnp.einsum(
            "mlt,mlk->mtk", legendre, mixed_coef, preferred_element_type=jnp.float32
        ).astype(jnp.bfloat16)
        synthesis = synthesis.reshape(orders, lats, rows_lat, 2 * groups).transpose(1, 0, 2, 3)
    synthesis = synthesis.reshape(lats * orders, rows_lat, 2 * groups)
    gridded = lax.all_to_all(synthesis, "lat", split_axis=0, concat_axis=0, tiled=True)
    spread = gridded.reshape(M, rows_lat, 2, groups)
    restored = jnp.einsum("mtrc,rmn->ctn", spread, fourier, preferred_element_type=jnp.float32)
    return (restored + grid_in.astype(jnp.float32)).astype(jnp.bfloat16)


MESH = pl.DeviceIdType.MESH
LANES = 128
TILE = 16
PAD = 1
AHEAD = 3
BEHIND = (1, 2)
VMEM_LIMIT = 67043328


def pitch_of(count):
    return count + PAD


def helped_from(lats):
    return max(lats // 2, lats - lats // 4)


def chunks_of(orders, chans):
    return next((count for count in (4, 3, 2, 1) if orders % (count * chans) == 0), 0)


def exchange_kernel(
    lats, chans, chunks,
    leg, grid, table, quad, mix, arrived, weights,
    field, turned, waves, w_send, w_recv, c_send, c_recv, x_recv, s_send,
    w_help, h_send, c_help, x_help, leg_help,
    legs, tiles, wide,
    leg_sem, tile_sem, own_sem, field_sem,
    ws_sem, wr_sem, cs_sem, cr_sem, xs_sem, xr_sem, ss_sem, sr_sem, gs_sem, gr_sem,
    wh_sem, hs_sem, hr_sem, ys_sem, yr_sem, zs_sem, ls_sem, lf_sem, lr_sem,
):
    here = lax.axis_index("lat")
    group = lax.axis_index("chan")
    orders, degrees_all, points_all = leg.shape
    degrees = degrees_all // lats
    points = points_all // lats
    size = orders // chunks
    part = size // chans
    rows = lats * part
    columns = w_send.shape[-1]
    _, groups, _, length = field.shape
    half = columns // 2
    folds = length // columns
    every = lats * size
    span = tiles.shape[1]
    bands = degrees // span
    inner = tiles.shape[3] // chans
    pitch = pitch_of(degrees)
    depth = rows * pitch
    mid = lats // 2
    wards, _, quarter = h_send.shape[:3]
    guard = lats - wards
    reach = leg_help.shape[2]
    ward = here + mid
    turn_of = ward - guard
    low = here < mid
    owning = here >= guard
    helping = jnp.logical_and(low, ward >= guard)
    batch = 256 // groups

    def to(lat, chan):
        return {"device_id": {"lat": lat, "chan": chan}, "device_id_type": MESH}

    def each_peer(do):
        def step(d, carry):
            do(lax.rem(here + d, lats))
            return carry

        lax.fori_loop(1, lats, step, 0)

    def each_pair(low, high, do):
        def step(n, carry):
            lat = n // chans
            chan = n % chans

            @pl.when(jnp.logical_or(lat != here, chan != group))
            def _():
                do(lat, chan)

            return carry

        lax.fori_loop(low * chans, high * chans, step, 0)

    def weighted_copy(j, peer, source):
        at = pl.ds(j * size, size)
        return pltpu.make_async_remote_copy(
            src_ref=w_send.at[peer, at], dst_ref=w_recv.at[source, at],
            send_sem=ws_sem.at[j, peer], recv_sem=wr_sem.at[j, source],
            **to(peer, group),
        )

    def helped_copy(j, peer, source):
        at = pl.ds(j * size, size)
        return pltpu.make_async_remote_copy(
            src_ref=w_send.at[peer, at], dst_ref=w_help.at[source, at],
            send_sem=ws_sem.at[j, peer], recv_sem=wh_sem.at[j, source],
            **to(peer - mid, group),
        )

    def weighted_to(j, peer, do):
        away = jnp.logical_and(low, peer >= guard)

        @pl.when(jnp.logical_and(jnp.logical_not(away), peer != here))
        def _():
            do(weighted_copy(j, peer, here))

        @pl.when(jnp.logical_and(away, peer - mid != here))
        def _():
            do(helped_copy(j, peer, here))

    def send_weighted(j):
        each_peer(lambda peer: weighted_to(j, peer, lambda copy: copy.start()))

    def sent_weighted(j):
        each_peer(lambda peer: weighted_to(j, peer, lambda copy: copy.wait_send()))

    def take_weighted(j):
        def take(source):
            @pl.when(jnp.logical_or(jnp.logical_not(owning), source >= mid))
            def _():
                weighted_copy(j, here, source).wait_recv()

        each_peer(take)

    def lane_of(count):
        return lax.broadcasted_iota(jnp.int32, (count, columns), 1) < half

    def field_copy(block):
        at = pl.ds(block * TILE, TILE)
        return pltpu.make_async_copy(grid.at[:, at], field.at[block % 2], field_sem.at[block % 2])

    def turn(block):
        pitch = pitch_of(TILE)
        count = groups * pitch

        def widen(c, carry):
            values = field[block % 2, c].astype(jnp.float32)
            for n in range(folds):
                wide[pl.ds(n * count + c * pitch, TILE), :] = values[:, n * columns : (n + 1) * columns]
            return carry

        lax.fori_loop(0, groups, widen, 0)

        def pick(t, carry):
            for n in range(folds):
                values = wide[pl.ds(n * count + t, groups, stride=pitch), :]
                turned[block * TILE + t, :, pl.ds(n * columns, columns)] = values.astype(jnp.bfloat16)
            return carry

        lax.fori_loop(0, TILE, pick, 0)

    def transform(j, send):
        lane = lane_of(every)
        at = pl.ds(j * every, every)
        lines = pl.ds(j * size, size)
        pitch = pitch_of(points)

        def step(b, carry):
            first = b * batch
            left = jnp.concatenate([waves[0, at], waves[1, at]], axis=0)
            right = turned[pl.ds(first, batch)].reshape(batch * groups, length)
            sums = lax.dot_general(left, right, (((1,), (1,)), ((), ())), preferred_element_type=jnp.float32)
            for pair in range(batch // 2):
                cut = slice(pair * columns, (pair + 1) * columns)
                real, imag = sums[:every, cut], sums[every:, cut]
                t = first + 2 * pair
                even = jnp.where(lane, real, pltpu.roll(imag, half, 1)) * quad[t]
                odd = jnp.where(lane, pltpu.roll(real, half, 1), imag) * quad[t + 1]
                wide[pl.ds(t, every, stride=pitch), :] = even
                wide[pl.ds(t + 1, every, stride=pitch), :] = odd
            return carry

        lax.fori_loop(0, points // batch, step, 0)

        def fold(d, carry):
            peer = lax.rem(here + d, lats)
            for n in range(size):
                values = wide[pl.ds((peer * size + n) * pitch, points), :]
                w_send[peer, j * size + n] = values.astype(jnp.bfloat16)

            if send:
                weighted_to(j, peer, lambda copy: copy.start())
            return carry

        lax.fori_loop(0, lats, fold, 0)
        w_recv[here, lines] = w_send[here, lines]

        @pl.when(helping)
        def _():
            w_help[here, lines] = w_send[ward, lines]


    def coeff_copy(j, lat, chan, from_lat, from_chan):
        at = pl.ds(j * part, part)
        return pltpu.make_async_remote_copy(
            src_ref=c_send.at[lat, chan, at], dst_ref=c_recv.at[from_lat, from_chan, at],
            send_sem=cs_sem.at[j, lat, chan], recv_sem=cr_sem.at[j, from_lat, from_chan],
            **to(lat, chan),
        )

    def mixed_copy(j, lat, chan, from_lat, from_chan):
        at = pl.ds(j * part, part)
        return pltpu.make_async_remote_copy(
            src_ref=c_send.at[slot_of(lat), chan, at], dst_ref=x_recv.at[from_lat, from_chan, at],
            send_sem=xs_sem.at[j, lat, chan], recv_sem=xr_sem.at[j, from_lat, from_chan],
            **to(lat, chan),
        )

    def slot_of(lat):
        return jnp.where(lat == here, lats, lat)

    def partial_copy(j, lat, chan, source, from_chan):
        at = pl.ds(j * part, part)
        return pltpu.make_async_remote_copy(
            src_ref=h_send.at[lat - guard, chan, at], dst_ref=c_help.at[source, from_chan, at],
            send_sem=hs_sem.at[j, lat - guard, chan], recv_sem=hr_sem.at[j, source, from_chan],
            **to(lat, chan),
        )

    def shared_copy(j, lat, chan, source, from_chan):
        at = pl.ds(j * part, part)
        return pltpu.make_async_remote_copy(
            src_ref=c_send.at[slot_of(lat), chan, at], dst_ref=x_help.at[source, from_chan, at],
            send_sem=ys_sem.at[j, lat - guard, chan], recv_sem=yr_sem.at[j, source, from_chan],
            **to(lat - mid, chan),
        )

    def every_pair(start, stop, do):
        def step(n, carry):
            do(n // chans, n % chans)
            return carry

        lax.fori_loop(start * chans, stop * chans, step, 0)

    def helper_copy(j, peer, block):
        at = pl.ds(j * size, size)
        return pltpu.make_async_remote_copy(
            src_ref=w_send.at[peer, at], dst_ref=arrived.at[block, at],
            send_sem=zs_sem.at[j, peer], recv_sem=sr_sem.at[j, block],
            **to(peer, group),
        )

    def each_low(do):
        def step(peer, carry):
            @pl.when(peer != here)
            def _():
                do(peer)

            return carry

        lax.fori_loop(0, mid, step, 0)

    def help_analyse(j):
        each_low(lambda source: helped_copy(j, ward, source).wait_recv())
        blank = jnp.zeros((reach - mid * points, columns), jnp.bfloat16)

        def step(n, carry):
            at = j * size + n
            values = jnp.concatenate([w_help[:, at].reshape(mid * points, columns), blank], axis=0)
            sums = jnp.dot(leg_help[at], values, preferred_element_type=jnp.float32)
            h_send[:, n // part, j * part + n % part] = sums.astype(jnp.bfloat16).reshape(wards, degrees, columns)
            return carry

        lax.fori_loop(0, size, step, 0)
        every_pair(ward, lats, lambda lat, chan: partial_copy(j, lat, chan, turn_of, group).start())

    def help_synthesise(j):
        every_pair(turn_of, wards, lambda block, chan: shared_copy(j, ward, group, block, chan).wait_recv())
        at = pl.ds(j * size, size)

        def step(n, carry):
            values = x_help[:, n // part, j * part + n % part].reshape(wards * degrees, columns)
            sums = lax.dot_general(
                leg_help[j * size + n], values, (((0,), (0,)), ((), ())), preferred_element_type=jnp.float32
            )
            sums = sums[: mid * points].astype(jnp.bfloat16).reshape(mid, points, columns)
            w_send[pl.ds(0, mid), j * size + n] = sums
            return carry

        lax.fori_loop(0, size, step, 0)
        each_low(lambda peer: helper_copy(j, peer, ward).start())
        keep = pltpu.make_async_copy(w_send.at[here, at], arrived.at[ward, at], own_sem.at[1])
        keep.start()
        keep.wait()

    def leg_share(block, lat, chan, source, send_sem):
        at = pl.ds(source * quarter, quarter)
        lines = pl.ds(block * degrees, (wards - block) * degrees)
        target = leg_help.at[at, lines]
        origin = target
        if send_sem is ls_sem:
            origin = leg.at[at, pl.ds((guard + block) * degrees, (wards - block) * degrees), pl.ds(0, reach)]
        return pltpu.make_async_remote_copy(
            src_ref=origin, dst_ref=target, send_sem=send_sem.at[chan], recv_sem=lr_sem.at[source],
            **to(lat, chan),
        )

    def each_ward(do):
        for block in range(wards):
            @pl.when(here == guard + block)
            def _():
                do(block, True)

            @pl.when(here == guard + block - mid)
            def _():
                do(block, False)

    def other_chans(do):
        def step(d, carry):
            do(lax.rem(group + d, chans))
            return carry

        lax.fori_loop(1, chans, step, 0)

    def legs_out(block, owner):
        if owner:
            leg_share(block, here - mid, group, group, ls_sem).start()
        elif block:
            cover = pl.ds(0, block * degrees)
            leg_help[:, cover, :] = jnp.zeros((orders, block * degrees, reach), jnp.bfloat16)
            x_help[pl.ds(0, block)] = jnp.zeros((block,) + x_help.shape[1:], x_help.dtype)

    def legs_on(block, owner):
        if not owner:
            leg_share(block, here, group, group, lf_sem).wait_recv()
            other_chans(lambda chan: leg_share(block, here, chan, group, lf_sem).start())

    def legs_in(block, owner):
        if not owner:
            other_chans(lambda chan: leg_share(block, here, group, chan, lf_sem).wait_recv())

    def legs_done(block, owner):
        if owner:
            leg_share(block, here - mid, group, group, ls_sem).wait_send()
        else:
            other_chans(lambda chan: leg_share(block, here, chan, group, lf_sem).wait_send())

    def synthesis_copy(j, peer, source):
        at = pl.ds(j * size, size)
        return pltpu.make_async_remote_copy(
            src_ref=s_send.at[peer, at], dst_ref=arrived.at[source, at],
            send_sem=ss_sem.at[j, peer], recv_sem=sr_sem.at[j, source],
            **to(peer, group),
        )

    def synthesis_to(peer, do):
        @pl.when(jnp.logical_or(jnp.logical_not(owning), peer >= mid))
        def _():
            do()

    def own_synthesis(j):
        at = pl.ds(j * size, size)
        return pltpu.make_async_copy(s_send.at[here, at], arrived.at[here, at], own_sem.at[1])

    def leg_copy(use, j):
        return pltpu.make_async_copy(leg.at[pl.ds(j * size, size)], legs.at[use % 2], leg_sem.at[use % 2])

    def analyse(use, j):
        def step(n, carry):
            at = j * size + n
            values = w_recv[:, at].reshape(lats * points, columns)
            sums = jnp.dot(legs[use % 2, n], values, preferred_element_type=jnp.float32)
            c_send[pl.ds(0, lats), n // part, j * part + n % part] = sums.astype(jnp.bfloat16).reshape(lats, degrees, columns)
            return carry

        lax.fori_loop(0, size, step, 0)
        at = pl.ds(j * part, part)
        each_pair(here, lats, lambda lat, chan: coeff_copy(j, lat, chan, here, group).start())
        c_recv[here, group, at] = c_send[here, group, at]

    def synthesise(use, j):
        def step(n, carry):
            values = x_recv[:, n // part, j * part + n % part].reshape(lats * degrees, columns)
            sums = lax.dot_general(
                legs[use % 2, n], values, (((0,), (0,)), ((), ())), preferred_element_type=jnp.float32
            )
            s_send[:, j * size + n] = sums.astype(jnp.bfloat16).reshape(lats, points, columns)
            return carry

        lax.fori_loop(0, size, step, 0)
        each_peer(lambda peer: synthesis_to(peer, lambda: synthesis_copy(j, peer, here).start()))
        own_synthesis(j).start()
        own_synthesis(j).wait()

    def tile_copies(band, slot, do):
        at = pl.ds(band * span, span)
        for chan in range(chans):
            for r in range(2):
                target = tiles.at[slot, :, r, pl.ds(chan * inner, inner)]
                sem = tile_sem.at[slot, chan, r]

                @pl.when(chan == group)
                def _():
                    do(pltpu.make_async_copy(mix.at[r, at], target, sem))

                @pl.when(chan != group)
                def _():
                    do(pltpu.make_async_copy(weights.at[chan, r, at], target, sem))

    def mix_chunk(j):
        at = pl.ds(j * part, part)
        tile_copies(0, 0, lambda copy: copy.start())

        def widen(s, carry):
            for chan in range(chans):
                for q in range(part):
                    values = c_recv[s, chan, j * part + q].astype(jnp.float32)
                    wide[pl.ds(chan * depth + (s * part + q) * pitch, degrees), :] = values
            return carry

        def widen_sum(s, carry):
            for chan in range(chans):
                for q in range(part):
                    values = c_recv[s, chan, j * part + q].astype(jnp.float32)
                    values += c_help[s - guard, chan, j * part + q].astype(jnp.float32)
                    wide[pl.ds(chan * depth + (s * part + q) * pitch, degrees), :] = values
            return carry

        lax.fori_loop(0, jnp.minimum(here + 1, guard), widen, 0)
        lax.fori_loop(guard, jnp.maximum(here + 1, guard), widen_sum, 0)
        lane = lane_of(rows)
        after = chans * depth

        def band_step(band, carry):
            slot = band % 2

            @pl.when(band + 1 < bands)
            def _():
                tile_copies(band + 1, 1 - slot, lambda copy: copy.start())

            tile_copies(band, slot, lambda copy: copy.wait())

            def degree_step(n, carry):
                line = band * span + n
                taken = [wide[pl.ds(chan * depth + line, rows, stride=pitch), :] for chan in range(chans)]
                real, imag = [], []
                for low, high in zip(taken[0::2], taken[1::2]):
                    real.append(jnp.where(lane, low, pltpu.roll(high, half, 1)))
                    imag.append(jnp.where(lane, pltpu.roll(low, half, 1), high))
                stacked = jnp.concatenate(
                    [jnp.concatenate(real, axis=1), jnp.concatenate(imag, axis=1)], axis=0
                ).astype(jnp.bfloat16)
                by_real = jnp.dot(stacked, tiles[slot, n, 0], preferred_element_type=jnp.float32)
                by_imag = jnp.dot(stacked, tiles[slot, n, 1], preferred_element_type=jnp.float32)
                real_out = by_real[:rows] - by_imag[rows:]
                imag_out = by_real[rows:] + by_imag[:rows]
                for pair in range(chans // 2):
                    first = real_out[:, pair * columns : (pair + 1) * columns]
                    second = imag_out[:, pair * columns : (pair + 1) * columns]
                    start = after + 2 * pair * depth + line
                    even = jnp.where(lane, first, pltpu.roll(second, half, 1))
                    odd = jnp.where(lane, pltpu.roll(first, half, 1), second)
                    wide[pl.ds(start, rows, stride=pitch), :] = even
                    wide[pl.ds(start + depth, rows, stride=pitch), :] = odd
                return carry

            lax.fori_loop(0, span, degree_step, 0)
            return carry

        lax.fori_loop(0, bands, band_step, 0)

        def narrow(s, carry):
            for chan in range(chans):
                for q in range(part):
                    values = wide[pl.ds(after + chan * depth + (s * part + q) * pitch, degrees), :]
                    c_send[slot_of(s), chan, j * part + q] = values.astype(jnp.bfloat16)
            return carry

        lax.fori_loop(0, here + 1, narrow, 0)
        each_pair(0, here + 1, lambda lat, chan: mixed_copy(j, lat, chan, here, group).start())
        every_pair(
            guard, jnp.maximum(here + 1, guard),
            lambda lat, chan: shared_copy(j, lat, chan, here - guard, group).start(),
        )
        x_recv[here, group, at] = c_send[lats, group, at]

    steps = []
    distance = chans // 2
    held = 1
    while distance:
        steps.append(distance)
        distance //= 2

    def gather_copies(level):
        distance = steps[level]
        peer = jnp.bitwise_xor(group, distance)
        copies = []
        for n in range(2**level):
            offset = sum(steps[b] for b in range(level) if n >> b & 1)
            shard = jnp.bitwise_xor(group, offset)
            source = mix if offset == 0 else weights.at[shard]
            copies.append(
                pltpu.make_async_remote_copy(
                    src_ref=source, dst_ref=weights.at[shard],
                    send_sem=gs_sem.at[level, n], recv_sem=gr_sem.at[level, n],
                    **to(here, peer),
                )
            )
        return copies

    plan = []
    for n in range(chunks + BEHIND[1]):
        for kind, lag in zip("LHXSG", (0, 0) + BEHIND + BEHIND[1:]):
            if 0 <= n - lag < chunks:
                plan.append((kind, n - lag))
    order = [(kind, j) for kind, j in plan if kind in "LS"]

    table_copy = pltpu.make_async_copy(table, waves, own_sem.at[0])
    blocks = points // TILE
    each_ward(legs_out)
    field_copy(0).start()
    table_copy.start()
    if blocks > 1:
        field_copy(1).start()
    leg_copy(0, order[0][1]).start()
    for copy in gather_copies(0):
        copy.start()
    for block in range(blocks):
        field_copy(block).wait()
        turn(block)
        if block + 2 < blocks:
            field_copy(block + 2).start()
    table_copy.wait()
    for j in range(chunks):
        transform(j, j < AHEAD)

    def clear(s, carry):
        x_recv[s] = jnp.zeros(x_recv.shape[1:], x_recv.dtype)
        return carry

    lax.fori_loop(0, here, clear, 0)

    @pl.when(owning)
    def _():
        for source in range(mid):
            w_recv[source] = jnp.zeros(w_recv.shape[1:], w_recv.dtype)

    each_ward(legs_on)

    use = 0
    gathered = False
    for kind, j in plan:
        if kind == "X":
            if not gathered:
                for level in range(len(steps)):
                    for copy in gather_copies(level):
                        copy.wait_recv()
                    if level + 1 < len(steps):
                        for copy in gather_copies(level + 1):
                            copy.start()
                gathered = True
            each_pair(0, here + 1, lambda lat, chan: coeff_copy(j, here, group, lat, chan).wait_recv())
            every_pair(
                guard, jnp.maximum(here + 1, guard),
                lambda lat, chan: partial_copy(j, here, group, lat - guard, chan).wait_recv(),
            )
            mix_chunk(j)
            continue
        if kind == "H":
            if j == 0:
                each_ward(legs_in)
            pl.when(helping)(functools.partial(help_analyse, j))
            continue
        if kind == "G":
            sent_weighted(j)
            pl.when(helping)(functools.partial(help_synthesise, j))
            continue
        if use + 1 < len(order):
            leg_copy(use + 1, order[use + 1][1]).start()
        if kind == "L":
            take_weighted(j)
            leg_copy(use, j).wait()
            analyse(use, j)
            if j + AHEAD < chunks:
                send_weighted(j + AHEAD)
        else:
            each_pair(here, lats, lambda lat, chan: mixed_copy(j, here, group, lat, chan).wait_recv())
            leg_copy(use, j).wait()
            synthesise(use, j)
        use += 1

    for level in range(len(steps)):
        for copy in gather_copies(level):
            copy.wait_send()
    each_ward(legs_done)
    for j in range(chunks):
        each_pair(here, lats, lambda lat, chan: coeff_copy(j, lat, chan, here, group).wait_send())
        each_pair(0, here + 1, lambda lat, chan: mixed_copy(j, lat, chan, here, group).wait_send())
        every_pair(
            guard, jnp.maximum(here + 1, guard),
            lambda lat, chan: shared_copy(j, lat, chan, here - guard, group).wait_send(),
        )

        @pl.when(helping)
        def _():
            every_pair(ward, lats, lambda lat, chan: partial_copy(j, lat, chan, turn_of, group).wait_send())

    for j in range(chunks):
        def take(block):
            @pl.when(jnp.logical_not(jnp.logical_and(helping, block == ward)))
            def _():
                synthesis_copy(j, here, block).wait_recv()

        each_peer(take)
        each_peer(lambda peer: synthesis_to(peer, lambda: synthesis_copy(j, peer, here).wait_send()))

        @pl.when(helping)
        def _():
            each_low(lambda peer: helper_copy(j, peer, ward).wait_send())


def exchange(chans, lats, chunks, legendre, grid_in, table, quad_weights, mixing):
    orders = legendre.shape[0]
    groups, points, length = grid_in.shape
    degrees = mixing.shape[1]
    columns = 2 * groups
    size = orders // chunks
    part = size // chans
    rows = lats * part
    span = next(count for count in (4, 3, 2, 1) if degrees % count == 0)
    wards = lats - helped_from(lats)
    reach = (lats // 2 * points + LANES - 1) // LANES * LANES
    inner = mixing.shape[2]
    levels = max(1, chans.bit_length() - 1)
    spectral = (lats, chans, orders // chans, degrees, columns)
    gridded = (lats, orders, points, columns)
    scratch = max(
        2 * chans * rows * pitch_of(degrees),
        lats * size * pitch_of(points),
        length // columns * groups * pitch_of(TILE),
    )
    half = jnp.bfloat16
    dma = pltpu.SemaphoreType.DMA
    anywhere = pl.BlockSpec(memory_space=pl.ANY)
    arrived, _ = pl.pallas_call(
        functools.partial(exchange_kernel, lats, chans, chunks),
        in_specs=[anywhere, anywhere, anywhere, pl.BlockSpec(memory_space=pltpu.SMEM), anywhere],
        out_specs=[anywhere] * 2,
        out_shape=[
            jax.ShapeDtypeStruct(gridded, half),
            jax.ShapeDtypeStruct((chans,) + mixing.shape, half),
        ],
        scratch_shapes=[
            pltpu.VMEM((2, groups, TILE, length), half),
            pltpu.VMEM((points, groups, length), half),
            pltpu.VMEM(table.shape, half),
            pltpu.VMEM(gridded, half),
            pltpu.VMEM(gridded, half),
            pltpu.VMEM((lats + 1,) + spectral[1:], half),
            pltpu.VMEM(spectral, half),
            pltpu.VMEM(spectral, half),
            pltpu.VMEM(gridded, half),
            pltpu.VMEM((lats // 2,) + gridded[1:], half),
            pltpu.VMEM((wards,) + spectral[1:], half),
            pltpu.VMEM((wards,) + spectral[1:], half),
            pltpu.VMEM((wards,) + spectral[1:], half),
            pltpu.VMEM((orders, wards * degrees, reach), half),
            pltpu.VMEM((2, size) + legendre.shape[1:], half),
            pltpu.VMEM((2, span, 2, chans * inner, mixing.shape[3]), half),
            pltpu.VMEM((scratch, columns), jnp.float32),
            dma((2,)),
            dma((2, chans, 2)),
            dma((2,)),
            dma((2,)),
            dma((chunks, lats)),
            dma((chunks, lats)),
            dma((chunks, lats, chans)),
            dma((chunks, lats, chans)),
            dma((chunks, lats, chans)),
            dma((chunks, lats, chans)),
            dma((chunks, lats)),
            dma((chunks, lats)),
            dma((levels, chans)),
            dma((levels, chans)),
            dma((chunks, lats // 2)),
            dma((chunks, wards, chans)),
            dma((chunks, wards, chans)),
            dma((chunks, wards, chans)),
            dma((chunks, wards, chans)),
            dma((chunks, lats // 2)),
            dma((chans,)),
            dma((chans,)),
            dma((chans,)),
        ],
        compiler_params=pltpu.CompilerParams(has_side_effects=True, vmem_limit_bytes=VMEM_LIMIT),
    )(legendre, grid_in, table, quad_weights, mixing)
    return arrived


def restore_kernel(chunks, spectra, grid, waves, out, lines, sums, left):
    lats, orders, tile, columns = spectra.shape
    groups, _, length = grid.shape
    size = orders // chunks
    total = lats * orders
    half = columns // 2
    folds = length // columns
    batch = 2 if folds % 2 == 0 else 1
    pitch = pitch_of(tile)
    count = groups * pitch
    lane = lax.broadcasted_iota(jnp.int32, (total, columns), 1) < half

    def widen(lat, carry):
        for chunk in range(chunks):
            for n in range(size):
                start = ((chunk * lats + lat) * size + n) * pitch
                lines[pl.ds(start, tile), :] = spectra[lat, chunk * size + n].astype(jnp.float32)
        return carry

    lax.fori_loop(0, lats, widen, 0)

    def pick(pair, carry):
        low = lines[pl.ds(2 * pair, total, stride=pitch), :]
        high = lines[pl.ds(2 * pair + 1, total, stride=pitch), :]
        real = jnp.where(lane, low, pltpu.roll(high, half, 1))
        imag = jnp.where(lane, pltpu.roll(low, half, 1), high)
        values = jnp.concatenate([real, imag], axis=0).T.astype(jnp.bfloat16)
        left[pl.ds(pair * columns, columns), :] = values
        return carry

    lax.fori_loop(0, tile // 2, pick, 0)

    def step(b, carry):
        cut = pl.ds(pl.multiple_of(b * batch * columns, batch * columns), batch * columns)
        right = waves[:, :, cut].reshape(2 * total, batch * columns)
        result = jnp.dot(left[...], right, preferred_element_type=jnp.float32)
        for t in range(tile):
            for n in range(batch):
                values = result[t * groups : (t + 1) * groups, n * columns : (n + 1) * columns]
                sums[pl.ds((b * batch + n) * count + t, groups, stride=pitch), :] = values
        return carry

    lax.fori_loop(0, folds // batch, step, 0)

    def add(c, carry):
        for n in range(folds):
            cut = pl.ds(n * columns, columns)
            values = sums[pl.ds(n * count + c * pitch, tile), :] + grid[c, :, cut].astype(jnp.float32)
            out[c, :, cut] = values.astype(jnp.bfloat16)
        return carry

    lax.fori_loop(0, groups, add, 0)


def restore(chunks, gridded, grid_in, table):
    lats, orders, points, columns = gridded.shape
    groups, _, length = grid_in.shape
    by_rows = pl.BlockSpec((groups, TILE, length), lambda g: (0, g, 0))
    return pl.pallas_call(
        functools.partial(restore_kernel, chunks),
        grid=(points // TILE,),
        in_specs=[
            pl.BlockSpec((lats, orders, TILE, columns), lambda g: (0, 0, g, 0)),
            by_rows,
            pl.BlockSpec(table.shape, lambda g: (0, 0, 0)),
        ],
        out_specs=by_rows,
        out_shape=jax.ShapeDtypeStruct(grid_in.shape, jnp.bfloat16),
        scratch_shapes=[
            pltpu.VMEM((lats * orders * pitch_of(TILE), columns), jnp.float32),
            pltpu.VMEM((length // columns * groups * pitch_of(TILE), columns), jnp.float32),
            pltpu.VMEM((groups * TILE, 2 * lats * orders), jnp.bfloat16),
        ],
        compiler_params=pltpu.CompilerParams(vmem_limit_bytes=VMEM_LIMIT),
    )(gridded, grid_in, table)


def wave_table(lats, orders, chunks, length):
    at = np.arange(lats * orders).reshape(lats, chunks, orders // chunks)
    phases = at.transpose(1, 0, 2).reshape(-1, 1) * np.arange(length)[None, :] % length
    angles = phases.astype(np.float32) * np.float32(2.0 * math.pi / length)
    values = np.stack([np.cos(angles), -np.sin(angles)]) * np.float32(1.0 / math.sqrt(length))
    return jnp.asarray(values.astype(jnp.bfloat16))


def body(chans, lats, grid_in, quad_weights, legendre, mixing):
    groups, rows_lat, length = grid_in.shape
    orders = legendre.shape[0]
    degrees = mixing.shape[1]
    chunks = chunks_of(orders, chans)
    fits = (
        chunks > 0
        and chans > 1
        and chans & (chans - 1) == 0
        and lats % 2 == 0
        and 2 * groups == LANES
        and rows_lat % TILE == 0
        and length % LANES == 0
        and degrees % TILE == 0
        and orders * lats == M
        and degrees * lats == legendre.shape[1]
        and lats * (orders // (chunks * chans)) % 8 == 0
    )
    if not fits:
        return general(chans, grid_in, quad_weights, legendre, mixing)
    table = wave_table(lats, orders, chunks, length)
    gridded = exchange(chans, lats, chunks, legendre, grid_in, table, quad_weights, mixing)
    return restore(chunks, gridded, grid_in, table)


def solution(mesh):
    return jax.shard_map(
        functools.partial(body, mesh.shape["chan"], mesh.shape["lat"]),
        mesh=mesh,
        in_specs=(
            P("chan", "lat", None),
            P("lat"),
            P("lat", None, None),
            P(None, "lat", "chan", None),
        ),
        out_specs=P("chan", "lat", None),
        check_vma=False,
    )
```

```python
import functools
import math

import jax
import jax.numpy as jnp
import numpy as np
from jax import lax
from jax.experimental import pallas as pl
from jax.experimental.pallas import tpu as pltpu
from jax.sharding import PartitionSpec as P

M = 384
PIECES = (2, 1)


def fourier_table(number, length):
    orders = jnp.arange(number, dtype=jnp.int32)
    points = jnp.arange(length, dtype=jnp.int32)
    phases = orders[:, None] * points[None, :] % length
    angles = phases.astype(jnp.float32) * (2.0 * math.pi / length)
    factor = 1.0 / math.sqrt(length)
    return jnp.stack([jnp.cos(angles) * factor, -jnp.sin(angles) * factor]).astype(jnp.bfloat16)


def step_of(part):
    return next(count for count in (4, 3, 2, 1) if part % count == 0)


def price(legendre, columns):
    orders, degrees, points = legendre.shape
    return pl.CostEstimate(
        flops=2 * orders * degrees * points * columns,
        bytes_accessed=2 * orders * (degrees * points + (degrees + points) * columns),
        transcendentals=0,
    )


def analyse(legendre, gathered, chans):
    lats, orders, rows_lat, columns = gathered.shape
    degrees = legendre.shape[1] // lats
    part = orders // chans
    step = step_of(part)
    runs = part // step

    def kernel(table_ref, values_ref, out_ref):
        for at in range(step):
            values = values_ref[:, at].reshape(lats * rows_lat, columns)
            sums = jnp.dot(table_ref[at], values, preferred_element_type=jnp.float32)
            out_ref[:, 0, at] = sums.astype(jnp.bfloat16).reshape(lats, degrees, columns)

    return pl.pallas_call(
        kernel,
        grid=(orders // step,),
        in_specs=[
            pl.BlockSpec((step,) + legendre.shape[1:], lambda g: (g, 0, 0)),
            pl.BlockSpec((lats, step, rows_lat, columns), lambda g: (0, g, 0, 0)),
        ],
        out_specs=pl.BlockSpec(
            (lats, 1, step, degrees, columns), lambda g: (0, g // runs, g % runs, 0, 0)
        ),
        out_shape=jax.ShapeDtypeStruct((lats, chans, part, degrees, columns), jnp.bfloat16),
        cost_estimate=price(legendre, columns),
    )(legendre, gathered)


def synthesise(legendre, returned, rows_lat):
    lats, chans, part, degrees, columns = returned.shape
    orders = legendre.shape[0]
    step = step_of(part)
    runs = part // step

    def kernel(table_ref, values_ref, out_ref):
        for at in range(step):
            values = values_ref[:, 0, at].reshape(lats * degrees, columns)
            sums = lax.dot_general(
                table_ref[at],
                values,
                (((0,), (0,)), ((), ())),
                preferred_element_type=jnp.float32,
            )
            out_ref[:, at] = sums.astype(jnp.bfloat16).reshape(lats, rows_lat, columns)

    return pl.pallas_call(
        kernel,
        grid=(orders // step,),
        in_specs=[
            pl.BlockSpec((step,) + legendre.shape[1:], lambda g: (g, 0, 0)),
            pl.BlockSpec(
                (lats, 1, step, degrees, columns), lambda g: (0, g // runs, g % runs, 0, 0)
            ),
        ],
        out_specs=pl.BlockSpec((lats, step, rows_lat, columns), lambda g: (0, g, 0, 0)),
        out_shape=jax.ShapeDtypeStruct((lats, orders, rows_lat, columns), jnp.bfloat16),
        cost_estimate=price(legendre, columns),
    )(legendre, returned)


def general(chans, grid_in, quad_weights, legendre, mixing):
    groups = grid_in.shape[0]
    rows_lat = grid_in.shape[1]
    length = grid_in.shape[2]
    orders = legendre.shape[0]
    degrees = mixing.shape[1]
    lats = legendre.shape[1] // degrees
    part = -(-orders // chans)
    padding = part * chans - orders
    everyone = ("lat", "chan")

    channel = jnp.arange(chans * groups)
    place = channel // groups * (2 * groups) + channel % groups
    column = jnp.arange(2 * chans * groups)
    to_real = (column == place[:, None]).astype(jnp.bfloat16)
    to_imag = (column == place[:, None] + groups).astype(jnp.bfloat16)

    def spread_out(table):
        return jnp.einsum(
            "rlcd,rdy->lcy", mixing, table, preferred_element_type=jnp.float32
        ).astype(jnp.bfloat16)

    blocks = jnp.concatenate(
        [
            spread_out(jnp.stack([to_real, to_imag])),
            spread_out(jnp.stack([to_imag, -to_real])),
        ],
        axis=1,
    )
    weights = lax.all_gather(blocks, "chan", axis=0)
    fourier = fourier_table(M, length)
    spectra = jnp.einsum("ctn,rmn->mtrc", grid_in, fourier, preferred_element_type=jnp.float32)
    spectra = spectra * quad_weights[None, :, None, None]
    weighted = spectra.astype(jnp.bfloat16).reshape(M, rows_lat, 2 * groups)
    gathered = lax.all_to_all(weighted, "lat", split_axis=0, concat_axis=0, tiled=True)
    gathered = gathered.reshape(lats, orders, rows_lat, 2 * groups)
    fits = padding == 0 and rows_lat % 16 == 0 and degrees % 16 == 0
    if fits:
        outgoing = analyse(legendre, gathered, chans)
    else:
        whole = gathered.transpose(1, 0, 2, 3).reshape(orders, lats * rows_lat, 2 * groups)
        coeffs = jnp.einsum(
            "mlt,mtk->mlk", legendre, whole, preferred_element_type=jnp.float32
        ).astype(jnp.bfloat16)
        coeffs = jnp.pad(coeffs, ((0, padding), (0, 0), (0, 0)))
        outgoing = coeffs.reshape(chans, part, lats, degrees, 2 * groups)
        outgoing = outgoing.transpose(2, 0, 1, 3, 4)
    pieces = next(count for count in PIECES if part % count == 0)
    width = part // pieces
    place_lat = lax.axis_index("lat")
    peers = jnp.arange(lats).reshape(lats, 1, 1, 1, 1)

    def exchange(buffer, axes):
        flat = buffer.reshape((-1,) + buffer.shape[-3:])
        flat = lax.all_to_all(flat, axes, split_axis=0, concat_axis=0, tiled=True)
        return flat.reshape(buffer.shape)

    def mix(arrived):
        mixed = jnp.einsum(
            "ikmlx,klxy->limy", arrived, weights, preferred_element_type=jnp.float32
        ).astype(jnp.bfloat16)
        mixed = mixed.reshape(degrees, lats, width, chans, 2 * groups)
        return mixed.transpose(1, 3, 2, 0, 4)

    received = [exchange(outgoing[:, :, :width], ("lat", "chan"))]
    own = []
    for piece in range(1, pieces + 1):
        mixed = mix(received[-1])
        if piece < pieces:
            own.append(lax.dynamic_index_in_dim(mixed, place_lat, 0, keepdims=False))
            coming = outgoing[:, :, piece * width : (piece + 1) * width]
            mixed = jnp.where(peers >= place_lat, coming, mixed)
        received.append(exchange(mixed, ("lat", "chan")))
    if own:
        own = exchange(jnp.concatenate(own, axis=1), "chan")
    returned = []
    for piece in range(pieces):
        block = received[piece + 1]
        if piece < pieces - 1:
            mine = own[None, :, piece * width : (piece + 1) * width]
            block = jnp.where(peers == place_lat, mine, block)
        returned.append(jnp.where(peers >= place_lat, block, jnp.zeros_like(block)))
    returned = jnp.concatenate(returned, axis=2)
    if fits:
        synthesis = synthesise(legendre, returned, rows_lat)
    else:
        mixed_coef = returned.transpose(1, 2, 0, 3, 4)
        mixed_coef = mixed_coef.reshape(chans * part, lats * degrees, 2 * groups)[:orders]
        synthesis = jnp.einsum(
            "mlt,mlk->mtk", legendre, mixed_coef, preferred_element_type=jnp.float32
        ).astype(jnp.bfloat16)
        synthesis = synthesis.reshape(orders, lats, rows_lat, 2 * groups).transpose(1, 0, 2, 3)
    synthesis = synthesis.reshape(lats * orders, rows_lat, 2 * groups)
    gridded = lax.all_to_all(synthesis, "lat", split_axis=0, concat_axis=0, tiled=True)
    spread = gridded.reshape(M, rows_lat, 2, groups)
    restored = jnp.einsum("mtrc,rmn->ctn", spread, fourier, preferred_element_type=jnp.float32)
    return (restored + grid_in.astype(jnp.float32)).astype(jnp.bfloat16)


MESH = pl.DeviceIdType.MESH
LANES = 128
TILE = 16
PAD = 1
SHARES = (3, 3, 3, 2, 1)
AHEAD = 3
BEHIND = (1, 2)
VMEM_LIMIT = 67043328


def pitch_of(count):
    return count + PAD


def helped_from(lats):
    return max(lats // 2, lats - lats // 4)


def sizes_of(orders, chans):
    if orders % chans:
        return ()
    units = orders // chans
    shares = SHARES
    total = sum(shares)
    ends = [units * sum(shares[: n + 1]) // total for n in range(len(shares))]
    counts = [end - begin for begin, end in zip([0] + ends, ends)]
    return tuple(chans * count for count in counts if count)


def exchange_kernel(
    lats, chans, sizes,
    leg, grid, table, quad, mix, arrived, weights,
    field, turned, waves, w_send, w_recv, c_send, c_recv, x_recv, s_send,
    w_help, h_send, c_help, x_help, leg_help,
    legs, tiles, wide,
    leg_sem, tile_sem, own_sem, field_sem,
    ws_sem, wr_sem, cs_sem, cr_sem, xs_sem, xr_sem, ss_sem, sr_sem, gs_sem, gr_sem,
    wh_sem, hs_sem, hr_sem, ys_sem, yr_sem, zs_sem, ls_sem, lf_sem, lr_sem,
):
    here = lax.axis_index("lat")
    group = lax.axis_index("chan")
    orders, degrees_all, points_all = leg.shape
    degrees = degrees_all // lats
    points = points_all // lats
    chunks = len(sizes)
    starts = [sum(sizes[:j]) for j in range(chunks)]
    parts = [count // chans for count in sizes]
    places = [start // chans for start in starts]
    columns = w_send.shape[-1]
    _, groups, _, length = field.shape
    half = columns // 2
    folds = length // columns
    span = tiles.shape[1]
    bands = degrees // span
    inner = tiles.shape[3] // chans
    pitch = pitch_of(degrees)
    mid = lats // 2
    wards, _, quarter = h_send.shape[:3]
    guard = lats - wards
    reach = leg_help.shape[2]
    ward = here + mid
    turn_of = ward - guard
    low = here < mid
    owning = here >= guard
    helping = jnp.logical_and(low, ward >= guard)
    batch = 256 // groups

    def to(lat, chan):
        return {"device_id": {"lat": lat, "chan": chan}, "device_id_type": MESH}

    def each_peer(do):
        def step(d, carry):
            do(lax.rem(here + d, lats))
            return carry

        lax.fori_loop(1, lats, step, 0)

    def each_pair(low, high, do, down=False):
        def step(n, carry):
            lat = low + high - 1 - n // chans if down else n // chans
            chan = n % chans

            @pl.when(jnp.logical_or(lat != here, chan != group))
            def _():
                do(lat, chan)

            return carry

        lax.fori_loop(low * chans, high * chans, step, 0)

    def weighted_copy(j, peer, source):
        at = pl.ds(starts[j], sizes[j])
        return pltpu.make_async_remote_copy(
            src_ref=w_send.at[peer, at], dst_ref=w_recv.at[source, at],
            send_sem=ws_sem.at[j, peer], recv_sem=wr_sem.at[j, source],
            **to(peer, group),
        )

    def helped_copy(j, peer, source):
        at = pl.ds(starts[j], sizes[j])
        return pltpu.make_async_remote_copy(
            src_ref=w_send.at[peer, at], dst_ref=w_help.at[source, at],
            send_sem=ws_sem.at[j, peer], recv_sem=wh_sem.at[j, source],
            **to(peer - mid, group),
        )

    def weighted_to(j, peer, do):
        away = jnp.logical_and(low, peer >= guard)

        @pl.when(jnp.logical_and(jnp.logical_not(away), peer != here))
        def _():
            do(weighted_copy(j, peer, here))

        @pl.when(jnp.logical_and(away, peer - mid != here))
        def _():
            do(helped_copy(j, peer, here))

    def send_weighted(j):
        each_peer(lambda peer: weighted_to(j, peer, lambda copy: copy.start()))

    def sent_weighted(j):
        each_peer(lambda peer: weighted_to(j, peer, lambda copy: copy.wait_send()))

    def take_weighted(j):
        def take(source):
            @pl.when(jnp.logical_or(jnp.logical_not(owning), source >= mid))
            def _():
                weighted_copy(j, here, source).wait_recv()

        each_peer(take)

    def lane_of(count):
        return lax.broadcasted_iota(jnp.int32, (count, columns), 1) < half

    def field_copy(block):
        at = pl.ds(block * TILE, TILE)
        return pltpu.make_async_copy(grid.at[:, at], field.at[block % 2], field_sem.at[block % 2])

    def turn(block):
        pitch = pitch_of(TILE)
        count = groups * pitch

        def widen(c, carry):
            values = field[block % 2, c].astype(jnp.float32)
            for n in range(folds):
                wide[pl.ds(n * count + c * pitch, TILE), :] = values[:, n * columns : (n + 1) * columns]
            return carry

        lax.fori_loop(0, groups, widen, 0)

        def pick(t, carry):
            for n in range(folds):
                values = wide[pl.ds(n * count + t, groups, stride=pitch), :]
                turned[block * TILE + t, :, pl.ds(n * columns, columns)] = values.astype(jnp.bfloat16)
            return carry

        lax.fori_loop(0, TILE, pick, 0)

    def transform(j, send):
        size = sizes[j]
        every = lats * size
        lane = lane_of(every)
        at = pl.ds(lats * starts[j], every)
        lines = pl.ds(starts[j], sizes[j])
        pitch = pitch_of(points)

        def step(b, carry):
            first = b * batch
            left = jnp.concatenate([waves[0, at], waves[1, at]], axis=0)
            right = turned[pl.ds(first, batch)].reshape(batch * groups, length)
            sums = lax.dot_general(left, right, (((1,), (1,)), ((), ())), preferred_element_type=jnp.float32)
            for pair in range(batch // 2):
                cut = slice(pair * columns, (pair + 1) * columns)
                real, imag = sums[:every, cut], sums[every:, cut]
                t = first + 2 * pair
                even = jnp.where(lane, real, pltpu.roll(imag, half, 1)) * quad[t]
                odd = jnp.where(lane, pltpu.roll(real, half, 1), imag) * quad[t + 1]
                wide[pl.ds(t, every, stride=pitch), :] = even
                wide[pl.ds(t + 1, every, stride=pitch), :] = odd
            return carry

        lax.fori_loop(0, points // batch, step, 0)

        def fold(d, carry):
            peer = lax.rem(here + d, lats)
            for n in range(size):
                values = wide[pl.ds((peer * size + n) * pitch, points), :]
                w_send[peer, starts[j] + n] = values.astype(jnp.bfloat16)

            if send:
                weighted_to(j, peer, lambda copy: copy.start())
            return carry

        lax.fori_loop(0, lats, fold, 0)
        w_recv[here, lines] = w_send[here, lines]

        @pl.when(helping)
        def _():
            w_help[here, lines] = w_send[ward, lines]


    def coeff_copy(j, lat, chan, from_lat, from_chan):
        at = pl.ds(places[j], parts[j])
        return pltpu.make_async_remote_copy(
            src_ref=c_send.at[lat, chan, at], dst_ref=c_recv.at[from_lat, from_chan, at],
            send_sem=cs_sem.at[j, lat, chan], recv_sem=cr_sem.at[j, from_lat, from_chan],
            **to(lat, chan),
        )

    def mixed_copy(j, lat, chan, from_lat, from_chan):
        at = pl.ds(places[j], parts[j])
        return pltpu.make_async_remote_copy(
            src_ref=c_send.at[slot_of(lat), chan, at], dst_ref=x_recv.at[from_lat, from_chan, at],
            send_sem=xs_sem.at[j, lat, chan], recv_sem=xr_sem.at[j, from_lat, from_chan],
            **to(lat, chan),
        )

    def slot_of(lat):
        return jnp.where(lat == here, lats, lat)

    def partial_copy(j, lat, chan, source, from_chan):
        at = pl.ds(places[j], parts[j])
        return pltpu.make_async_remote_copy(
            src_ref=h_send.at[lat - guard, chan, at], dst_ref=c_help.at[source, from_chan, at],
            send_sem=hs_sem.at[j, lat - guard, chan], recv_sem=hr_sem.at[j, source, from_chan],
            **to(lat, chan),
        )

    def shared_copy(j, lat, chan, source, from_chan):
        at = pl.ds(places[j], parts[j])
        return pltpu.make_async_remote_copy(
            src_ref=c_send.at[slot_of(lat), chan, at], dst_ref=x_help.at[source, from_chan, at],
            send_sem=ys_sem.at[j, lat - guard, chan], recv_sem=yr_sem.at[j, source, from_chan],
            **to(lat - mid, chan),
        )

    def every_pair(start, stop, do):
        def step(n, carry):
            do(n // chans, n % chans)
            return carry

        lax.fori_loop(start * chans, stop * chans, step, 0)

    def helper_copy(j, peer, block):
        at = pl.ds(starts[j], sizes[j])
        return pltpu.make_async_remote_copy(
            src_ref=w_send.at[peer, at], dst_ref=arrived.at[block, at],
            send_sem=zs_sem.at[j, peer], recv_sem=sr_sem.at[j, block],
            **to(peer, group),
        )

    def each_low(do):
        def step(peer, carry):
            @pl.when(peer != here)
            def _():
                do(peer)

            return carry

        lax.fori_loop(0, mid, step, 0)

    def help_analyse(j):
        each_low(lambda source: helped_copy(j, ward, source).wait_recv())
        blank = jnp.zeros((reach - mid * points, columns), jnp.bfloat16)

        def step(n, carry):
            at = starts[j] + n
            values = jnp.concatenate([w_help[:, at].reshape(mid * points, columns), blank], axis=0)
            sums = jnp.dot(leg_help[at], values, preferred_element_type=jnp.float32)
            h_send[:, n // parts[j], places[j] + n % parts[j]] = sums.astype(jnp.bfloat16).reshape(wards, degrees, columns)
            return carry

        lax.fori_loop(0, sizes[j], step, 0)
        every_pair(ward, lats, lambda lat, chan: partial_copy(j, lat, chan, turn_of, group).start())

    def help_synthesise(j):
        every_pair(turn_of, wards, lambda block, chan: shared_copy(j, ward, group, block, chan).wait_recv())
        at = pl.ds(starts[j], sizes[j])

        def step(n, carry):
            values = x_help[:, n // parts[j], places[j] + n % parts[j]].reshape(wards * degrees, columns)
            sums = lax.dot_general(
                leg_help[starts[j] + n], values, (((0,), (0,)), ((), ())), preferred_element_type=jnp.float32
            )
            sums = sums[: mid * points].astype(jnp.bfloat16).reshape(mid, points, columns)
            w_send[pl.ds(0, mid), starts[j] + n] = sums
            return carry

        lax.fori_loop(0, sizes[j], step, 0)
        each_low(lambda peer: helper_copy(j, peer, ward).start())
        keep = pltpu.make_async_copy(w_send.at[here, at], arrived.at[ward, at], own_sem.at[1])
        keep.start()
        keep.wait()

    def leg_share(block, lat, chan, source, send_sem):
        at = pl.ds(source * quarter, quarter)
        lines = pl.ds(block * degrees, (wards - block) * degrees)
        target = leg_help.at[at, lines]
        origin = target
        if send_sem is ls_sem:
            origin = leg.at[at, pl.ds((guard + block) * degrees, (wards - block) * degrees), pl.ds(0, reach)]
        return pltpu.make_async_remote_copy(
            src_ref=origin, dst_ref=target, send_sem=send_sem.at[chan], recv_sem=lr_sem.at[source],
            **to(lat, chan),
        )

    def each_ward(do):
        for block in range(wards):
            @pl.when(here == guard + block)
            def _():
                do(block, True)

            @pl.when(here == guard + block - mid)
            def _():
                do(block, False)

    def other_chans(do):
        def step(d, carry):
            do(lax.rem(group + d, chans))
            return carry

        lax.fori_loop(1, chans, step, 0)

    def legs_out(block, owner):
        if owner:
            leg_share(block, here - mid, group, group, ls_sem).start()
        elif block:
            cover = pl.ds(0, block * degrees)
            leg_help[:, cover, :] = jnp.zeros((orders, block * degrees, reach), jnp.bfloat16)
            x_help[pl.ds(0, block)] = jnp.zeros((block,) + x_help.shape[1:], x_help.dtype)

    def legs_on(block, owner):
        if not owner:
            leg_share(block, here, group, group, lf_sem).wait_recv()
            other_chans(lambda chan: leg_share(block, here, chan, group, lf_sem).start())

    def legs_in(block, owner):
        if not owner:
            other_chans(lambda chan: leg_share(block, here, group, chan, lf_sem).wait_recv())

    def legs_done(block, owner):
        if owner:
            leg_share(block, here - mid, group, group, ls_sem).wait_send()
        else:
            other_chans(lambda chan: leg_share(block, here, chan, group, lf_sem).wait_send())

    def synthesis_copy(j, peer, source):
        at = pl.ds(starts[j], sizes[j])
        return pltpu.make_async_remote_copy(
            src_ref=s_send.at[peer, at], dst_ref=arrived.at[source, at],
            send_sem=ss_sem.at[j, peer], recv_sem=sr_sem.at[j, source],
            **to(peer, group),
        )

    def synthesis_to(peer, do):
        @pl.when(jnp.logical_or(jnp.logical_not(owning), peer >= mid))
        def _():
            do()

    def own_synthesis(j):
        at = pl.ds(starts[j], sizes[j])
        return pltpu.make_async_copy(s_send.at[here, at], arrived.at[here, at], own_sem.at[1])

    def leg_copy(use, j):
        return pltpu.make_async_copy(leg.at[pl.ds(starts[j], sizes[j])], legs.at[use % 2, pl.ds(0, sizes[j])], leg_sem.at[use % 2])

    def analyse(use, j):
        def step(n, carry):
            at = starts[j] + n
            values = w_recv[:, at].reshape(lats * points, columns)
            sums = jnp.dot(legs[use % 2, n], values, preferred_element_type=jnp.float32)
            c_send[pl.ds(0, lats), n // parts[j], places[j] + n % parts[j]] = sums.astype(jnp.bfloat16).reshape(lats, degrees, columns)
            return carry

        lax.fori_loop(0, sizes[j], step, 0)
        at = pl.ds(places[j], parts[j])
        each_pair(here, lats, lambda lat, chan: coeff_copy(j, lat, chan, here, group).start())
        c_recv[here, group, at] = c_send[here, group, at]

    def synthesise(use, j):
        def step(n, carry):
            values = x_recv[:, n // parts[j], places[j] + n % parts[j]].reshape(lats * degrees, columns)
            sums = lax.dot_general(
                legs[use % 2, n], values, (((0,), (0,)), ((), ())), preferred_element_type=jnp.float32
            )
            s_send[:, starts[j] + n] = sums.astype(jnp.bfloat16).reshape(lats, points, columns)
            return carry

        lax.fori_loop(0, sizes[j], step, 0)
        each_peer(lambda peer: synthesis_to(peer, lambda: synthesis_copy(j, peer, here).start()))
        own_synthesis(j).start()
        own_synthesis(j).wait()

    def tile_copies(band, slot, do):
        at = pl.ds(band * span, span)
        for chan in range(chans):
            for r in range(2):
                target = tiles.at[slot, :, r, pl.ds(chan * inner, inner)]
                sem = tile_sem.at[slot, chan, r]

                @pl.when(chan == group)
                def _():
                    do(pltpu.make_async_copy(mix.at[r, at], target, sem))

                @pl.when(chan != group)
                def _():
                    do(pltpu.make_async_copy(weights.at[chan, r, at], target, sem))

    def mix_chunk(j):
        part = parts[j]
        rows = lats * part
        depth = rows * pitch
        at = pl.ds(places[j], parts[j])
        tile_copies(0, 0, lambda copy: copy.start())

        def widen(s, carry):
            for chan in range(chans):
                for q in range(part):
                    values = c_recv[s, chan, places[j] + q].astype(jnp.float32)
                    wide[pl.ds(chan * depth + (s * part + q) * pitch, degrees), :] = values
            return carry

        def widen_sum(s, carry):
            for chan in range(chans):
                for q in range(part):
                    values = c_recv[s, chan, places[j] + q].astype(jnp.float32)
                    values += c_help[s - guard, chan, places[j] + q].astype(jnp.float32)
                    wide[pl.ds(chan * depth + (s * part + q) * pitch, degrees), :] = values
            return carry

        lax.fori_loop(0, jnp.minimum(here + 1, guard), widen, 0)
        lax.fori_loop(guard, jnp.maximum(here + 1, guard), widen_sum, 0)
        lane = lane_of(rows)
        after = chans * depth

        def band_step(band, carry):
            slot = band % 2

            @pl.when(band + 1 < bands)
            def _():
                tile_copies(band + 1, 1 - slot, lambda copy: copy.start())

            tile_copies(band, slot, lambda copy: copy.wait())

            def degree_step(n, carry):
                line = band * span + n
                taken = [wide[pl.ds(chan * depth + line, rows, stride=pitch), :] for chan in range(chans)]
                real, imag = [], []
                for low, high in zip(taken[0::2], taken[1::2]):
                    real.append(jnp.where(lane, low, pltpu.roll(high, half, 1)))
                    imag.append(jnp.where(lane, pltpu.roll(low, half, 1), high))
                stacked = jnp.concatenate(
                    [jnp.concatenate(real, axis=1), jnp.concatenate(imag, axis=1)], axis=0
                ).astype(jnp.bfloat16)
                by_real = jnp.dot(stacked, tiles[slot, n, 0], preferred_element_type=jnp.float32)
                by_imag = jnp.dot(stacked, tiles[slot, n, 1], preferred_element_type=jnp.float32)
                real_out = by_real[:rows] - by_imag[rows:]
                imag_out = by_real[rows:] + by_imag[:rows]
                for pair in range(chans // 2):
                    first = real_out[:, pair * columns : (pair + 1) * columns]
                    second = imag_out[:, pair * columns : (pair + 1) * columns]
                    start = after + 2 * pair * depth + line
                    even = jnp.where(lane, first, pltpu.roll(second, half, 1))
                    odd = jnp.where(lane, pltpu.roll(first, half, 1), second)
                    wide[pl.ds(start, rows, stride=pitch), :] = even
                    wide[pl.ds(start + depth, rows, stride=pitch), :] = odd
                return carry

            lax.fori_loop(0, span, degree_step, 0)
            return carry

        lax.fori_loop(0, bands, band_step, 0)

        def narrow(s, carry):
            for chan in range(chans):
                for q in range(part):
                    values = wide[pl.ds(after + chan * depth + (s * part + q) * pitch, degrees), :]
                    c_send[slot_of(s), chan, places[j] + q] = values.astype(jnp.bfloat16)
            return carry

        lax.fori_loop(0, here + 1, narrow, 0)
        each_pair(0, here + 1, lambda lat, chan: mixed_copy(j, lat, chan, here, group).start(), True)
        every_pair(
            guard, jnp.maximum(here + 1, guard),
            lambda lat, chan: shared_copy(j, lat, chan, here - guard, group).start(),
        )
        x_recv[here, group, at] = c_send[lats, group, at]

    steps = []
    distance = chans // 2
    held = 1
    while distance:
        steps.append(distance)
        distance //= 2

    def gather_copies(level):
        distance = steps[level]
        peer = jnp.bitwise_xor(group, distance)
        copies = []
        for n in range(2**level):
            offset = sum(steps[b] for b in range(level) if n >> b & 1)
            shard = jnp.bitwise_xor(group, offset)
            source = mix if offset == 0 else weights.at[shard]
            copies.append(
                pltpu.make_async_remote_copy(
                    src_ref=source, dst_ref=weights.at[shard],
                    send_sem=gs_sem.at[level, n], recv_sem=gr_sem.at[level, n],
                    **to(here, peer),
                )
            )
        return copies

    plan = []
    for n in range(chunks + BEHIND[1]):
        for kind, lag in zip("LHXSG", (0, 0) + BEHIND + BEHIND[1:]):
            if 0 <= n - lag < chunks:
                plan.append((kind, n - lag))
    order = [(kind, j) for kind, j in plan if kind in "LS"]

    table_copy = pltpu.make_async_copy(table, waves, own_sem.at[0])
    blocks = points // TILE
    each_ward(legs_out)
    field_copy(0).start()
    table_copy.start()
    if blocks > 1:
        field_copy(1).start()
    leg_copy(0, order[0][1]).start()
    for copy in gather_copies(0):
        copy.start()
    for block in range(blocks):
        field_copy(block).wait()
        turn(block)
        if block + 2 < blocks:
            field_copy(block + 2).start()
    table_copy.wait()
    for j in range(chunks):
        transform(j, j < AHEAD)

    def clear(s, carry):
        x_recv[s] = jnp.zeros(x_recv.shape[1:], x_recv.dtype)
        return carry

    lax.fori_loop(0, here, clear, 0)

    @pl.when(owning)
    def _():
        for source in range(mid):
            w_recv[source] = jnp.zeros(w_recv.shape[1:], w_recv.dtype)

    each_ward(legs_on)

    use = 0
    gathered = False
    for kind, j in plan:
        if kind == "X":
            if not gathered:
                for level in range(len(steps)):
                    for copy in gather_copies(level):
                        copy.wait_recv()
                    if level + 1 < len(steps):
                        for copy in gather_copies(level + 1):
                            copy.start()
                gathered = True
            each_pair(0, here + 1, lambda lat, chan: coeff_copy(j, here, group, lat, chan).wait_recv())
            every_pair(
                guard, jnp.maximum(here + 1, guard),
                lambda lat, chan: partial_copy(j, here, group, lat - guard, chan).wait_recv(),
            )
            mix_chunk(j)
            continue
        if kind == "H":
            if j == 0:
                each_ward(legs_in)
            pl.when(helping)(functools.partial(help_analyse, j))
            continue
        if kind == "G":
            sent_weighted(j)
            pl.when(helping)(functools.partial(help_synthesise, j))
            continue
        if use + 1 < len(order):
            leg_copy(use + 1, order[use + 1][1]).start()
        if kind == "L":
            take_weighted(j)
            leg_copy(use, j).wait()
            analyse(use, j)
            if j + AHEAD < chunks:
                send_weighted(j + AHEAD)
        else:
            each_pair(here, lats, lambda lat, chan: mixed_copy(j, here, group, lat, chan).wait_recv())
            leg_copy(use, j).wait()
            synthesise(use, j)
        use += 1

    for level in range(len(steps)):
        for copy in gather_copies(level):
            copy.wait_send()
    each_ward(legs_done)
    for j in range(chunks):
        each_pair(here, lats, lambda lat, chan: coeff_copy(j, lat, chan, here, group).wait_send())
        each_pair(0, here + 1, lambda lat, chan: mixed_copy(j, lat, chan, here, group).wait_send())
        every_pair(
            guard, jnp.maximum(here + 1, guard),
            lambda lat, chan: shared_copy(j, lat, chan, here - guard, group).wait_send(),
        )

        @pl.when(helping)
        def _():
            every_pair(ward, lats, lambda lat, chan: partial_copy(j, lat, chan, turn_of, group).wait_send())

    for j in range(chunks):
        def take(block):
            @pl.when(jnp.logical_not(jnp.logical_and(helping, block == ward)))
            def _():
                synthesis_copy(j, here, block).wait_recv()

        each_peer(take)
        each_peer(lambda peer: synthesis_to(peer, lambda: synthesis_copy(j, peer, here).wait_send()))

        @pl.when(helping)
        def _():
            each_low(lambda peer: helper_copy(j, peer, ward).wait_send())


def exchange(chans, lats, sizes, legendre, grid_in, table, quad_weights, mixing):
    orders = legendre.shape[0]
    groups, points, length = grid_in.shape
    degrees = mixing.shape[1]
    columns = 2 * groups
    chunks = len(sizes)
    size = max(sizes)
    rows = lats * (size // chans)
    span = next(count for count in (4, 3, 2, 1) if degrees % count == 0)
    wards = lats - helped_from(lats)
    reach = (lats // 2 * points + LANES - 1) // LANES * LANES
    inner = mixing.shape[2]
    levels = max(1, chans.bit_length() - 1)
    spectral = (lats, chans, orders // chans, degrees, columns)
    gridded = (lats, orders, points, columns)
    scratch = max(
        2 * chans * rows * pitch_of(degrees),
        lats * size * pitch_of(points),
        length // columns * groups * pitch_of(TILE),
    )
    half = jnp.bfloat16
    dma = pltpu.SemaphoreType.DMA
    anywhere = pl.BlockSpec(memory_space=pl.ANY)
    arrived, _ = pl.pallas_call(
        functools.partial(exchange_kernel, lats, chans, sizes),
        in_specs=[anywhere, anywhere, anywhere, pl.BlockSpec(memory_space=pltpu.SMEM), anywhere],
        out_specs=[anywhere] * 2,
        out_shape=[
            jax.ShapeDtypeStruct(gridded, half),
            jax.ShapeDtypeStruct((chans,) + mixing.shape, half),
        ],
        scratch_shapes=[
            pltpu.VMEM((2, groups, TILE, length), half),
            pltpu.VMEM((points, groups, length), half),
            pltpu.VMEM(table.shape, half),
            pltpu.VMEM(gridded, half),
            pltpu.VMEM(gridded, half),
            pltpu.VMEM((lats + 1,) + spectral[1:], half),
            pltpu.VMEM(spectral, half),
            pltpu.VMEM(spectral, half),
            pltpu.VMEM(gridded, half),
            pltpu.VMEM((lats // 2,) + gridded[1:], half),
            pltpu.VMEM((wards,) + spectral[1:], half),
            pltpu.VMEM((wards,) + spectral[1:], half),
            pltpu.VMEM((wards,) + spectral[1:], half),
            pltpu.VMEM((orders, wards * degrees, reach), half),
            pltpu.VMEM((2, size) + legendre.shape[1:], half),
            pltpu.VMEM((2, span, 2, chans * inner, mixing.shape[3]), half),
            pltpu.VMEM((scratch, columns), jnp.float32),
            dma((2,)),
            dma((2, chans, 2)),
            dma((2,)),
            dma((2,)),
            dma((chunks, lats)),
            dma((chunks, lats)),
            dma((chunks, lats, chans)),
            dma((chunks, lats, chans)),
            dma((chunks, lats, chans)),
            dma((chunks, lats, chans)),
            dma((chunks, lats)),
            dma((chunks, lats)),
            dma((levels, chans)),
            dma((levels, chans)),
            dma((chunks, lats // 2)),
            dma((chunks, wards, chans)),
            dma((chunks, wards, chans)),
            dma((chunks, wards, chans)),
            dma((chunks, wards, chans)),
            dma((chunks, lats // 2)),
            dma((chans,)),
            dma((chans,)),
            dma((chans,)),
        ],
        compiler_params=pltpu.CompilerParams(has_side_effects=True, vmem_limit_bytes=VMEM_LIMIT),
    )(legendre, grid_in, table, quad_weights, mixing)
    return arrived


def restore_kernel(sizes, spectra, grid, waves, out, lines, sums):
    lats, orders, tile, columns = spectra.shape
    groups, _, length = grid.shape
    total = lats * orders
    half = columns // 2
    folds = length // columns
    batch = 8
    pitch = pitch_of(tile)
    count = groups * pitch
    lane = lax.broadcasted_iota(jnp.int32, (total, columns), 1) < half

    def widen(lat, carry):
        first = 0
        for size in sizes:
            for n in range(size):
                start = (lats * first + lat * size + n) * pitch
                lines[pl.ds(start, tile), :] = spectra[lat, first + n].astype(jnp.float32)
            first += size
        return carry

    lax.fori_loop(0, lats, widen, 0)

    def step(b, carry):
        first = b * batch
        real, imag = [], []
        for pair in range(batch // 2):
            t = first + 2 * pair
            low = lines[pl.ds(t, total, stride=pitch), :]
            high = lines[pl.ds(t + 1, total, stride=pitch), :]
            real.append(jnp.where(lane, low, pltpu.roll(high, half, 1)))
            imag.append(jnp.where(lane, pltpu.roll(low, half, 1), high))
        left = jnp.concatenate([jnp.concatenate(real, axis=1), jnp.concatenate(imag, axis=1)], axis=0)
        result = lax.dot_general(
            left.astype(jnp.bfloat16), waves[...].reshape(2 * total, length),
            (((0,), (0,)), ((), ())), preferred_element_type=jnp.float32,
        )
        for t in range(batch):
            for n in range(folds):
                values = result[t * groups : (t + 1) * groups, n * columns : (n + 1) * columns]
                sums[pl.ds(n * count + first + t, groups, stride=pitch), :] = values
        return carry

    lax.fori_loop(0, tile // batch, step, 0)

    def add(c, carry):
        for n in range(folds):
            cut = pl.ds(n * columns, columns)
            values = sums[pl.ds(n * count + c * pitch, tile), :] + grid[c, :, cut].astype(jnp.float32)
            out[c, :, cut] = values.astype(jnp.bfloat16)
        return carry

    lax.fori_loop(0, groups, add, 0)


def restore(sizes, gridded, grid_in, table):
    lats, orders, points, columns = gridded.shape
    groups, _, length = grid_in.shape
    by_rows = pl.BlockSpec((groups, TILE, length), lambda g: (0, g, 0))
    return pl.pallas_call(
        functools.partial(restore_kernel, sizes),
        grid=(points // TILE,),
        in_specs=[
            pl.BlockSpec((lats, orders, TILE, columns), lambda g: (0, 0, g, 0)),
            by_rows,
            pl.BlockSpec(table.shape, lambda g: (0, 0, 0)),
        ],
        out_specs=by_rows,
        out_shape=jax.ShapeDtypeStruct(grid_in.shape, jnp.bfloat16),
        scratch_shapes=[
            pltpu.VMEM((lats * orders * pitch_of(TILE), columns), jnp.float32),
            pltpu.VMEM((length // columns * groups * pitch_of(TILE), columns), jnp.float32),
        ],
        compiler_params=pltpu.CompilerParams(vmem_limit_bytes=VMEM_LIMIT),
    )(gridded, grid_in, table)


def wave_table(lats, orders, sizes, length):
    at = np.arange(lats * orders).reshape(lats, orders)
    cuts = np.split(at, np.cumsum(sizes)[:-1], axis=1)
    at = np.concatenate([cut.reshape(-1) for cut in cuts])
    phases = at[:, None] * np.arange(length)[None, :] % length
    angles = phases.astype(np.float32) * np.float32(2.0 * math.pi / length)
    values = np.stack([np.cos(angles), -np.sin(angles)]) * np.float32(1.0 / math.sqrt(length))
    return jnp.asarray(values.astype(jnp.bfloat16))


def body(chans, lats, grid_in, quad_weights, legendre, mixing):
    groups, rows_lat, length = grid_in.shape
    orders = legendre.shape[0]
    degrees = mixing.shape[1]
    sizes = sizes_of(orders, chans)
    fits = (
        len(sizes) > 0
        and chans > 1
        and chans & (chans - 1) == 0
        and lats % 2 == 0
        and 2 * groups == LANES
        and rows_lat % TILE == 0
        and length % LANES == 0
        and degrees % TILE == 0
        and orders * lats == M
        and degrees * lats == legendre.shape[1]
        and lats % 8 == 0
    )
    if not fits:
        return general(chans, grid_in, quad_weights, legendre, mixing)
    table = wave_table(lats, orders, sizes, length)
    gridded = exchange(chans, lats, sizes, legendre, grid_in, table, quad_weights, mixing)
    return restore(sizes, gridded, grid_in, table)


def solution(mesh):
    return jax.shard_map(
        functools.partial(body, mesh.shape["chan"], mesh.shape["lat"]),
        mesh=mesh,
        in_specs=(
            P("chan", "lat", None),
            P("lat"),
            P("lat", None, None),
            P(None, "lat", "chan", None),
        ),
        out_specs=P("chan", "lat", None),
        check_vma=False,
    )
```
